32 devices in a mesh: col: 8 (over z, y), row: 4 (over x, core).
Axes of the slice: x: 2, y: 2, z: 4, core: 2. Of those that a mesh axis runs over, the one named last changes fastest.
Arguments:
- x_in: bfloat16 [2, 192, 1536, 128], P(None, 'row', 'col')
- a_pre: bfloat16 [2, 192, 1536, 128], P(None, 'row', 'col')
- g_out: bfloat16 [2, 192, 1536, 128], P(None, 'row', 'col')
- w_one: bfloat16 [3, 3, 128, 128], replicated
- w_two: bfloat16 [3, 3, 128, 128], replicated
Outputs:
- output 1: bfloat16 [2, 192, 1536, 128], P(None, 'row', 'col')
- output 2: float32 [3, 3, 128, 128], replicated
- output 3: float32 [3, 3, 128, 128], replicated
All inputs are finite; a program needn't handle non-finite values.
Results may differ from the reference program's by a relative error of at most 0.001.
Values are sent between devices in bfloat16 or wider.
A program may use at most 1 GiB of HBM per device.

```python
import jax
import jax.numpy as jnp
from jax import lax

IMAGES = 2
CHANNELS = 128
TILE_ROWS = 48
TILE_COLS = 192
IMG_HEIGHT = 192
IMG_WIDTH = 1536

FRAME_PAD = ((0, 0), (1, 1), (1, 1), (0, 0))


def conv_same(image_in, kernel):
    return lax.conv_general_dilated(image_in, kernel, (1, 1), "SAME", dimension_numbers=("NHWC", "HWIO", "NHWC"))


def gelu_slope(pre_act):
    tanh_scale = 0.7978845608028654
    cube_coef = 0.044715
    tanh_val = jnp.tanh(tanh_scale * (pre_act + cube_coef * pre_act * pre_act * pre_act))
    return 0.5 * (1.0 + tanh_val) + 0.5 * pre_act * (1.0 - tanh_val * tanh_val) * tanh_scale * (1.0 + 3.0 * cube_coef * pre_act * pre_act)


def tap_grads(left_pad, right_img):
    row_count = right_img.shape[1]
    col_count = right_img.shape[2]
    return jnp.stack([jnp.stack([jnp.einsum("bhwi,bhwo->io", left_pad[:, tap_row:tap_row + row_count, tap_col:tap_col + col_count], right_img) for tap_col in range(3)]) for tap_row in range(3)])


def edge_weight(boost):
    row_pos = jnp.arange(IMG_HEIGHT) % TILE_ROWS
    col_pos = jnp.arange(IMG_WIDTH) % TILE_COLS
    row_edge = (row_pos == 0) | (row_pos == TILE_ROWS - 1)
    col_edge = (col_pos == 0) | (col_pos == TILE_COLS - 1)
    on_edge = (row_edge[:, None] | col_edge[None, :]).astype(jnp.float32)
    return (1.0 + boost * on_edge)[None, :, :, None]


def setup_inputs(seed: int = 0) -> dict:
    key = jax.random.key(seed)
    key_x, key_a, key_g, key_one, key_two = jax.random.split(key, 5)
    img_shape = (IMAGES, IMG_HEIGHT, IMG_WIDTH, CHANNELS)
    fan_scale = (9 * CHANNELS) ** -0.5
    x_in = jax.random.normal(key_x, img_shape, jnp.float32).astype(jnp.bfloat16)
    a_pre = jax.random.normal(key_a, img_shape, jnp.float32).astype(jnp.bfloat16)
    g_out = (jax.random.normal(key_g, img_shape, jnp.float32) * edge_weight(2.0)).astype(jnp.bfloat16)
    w_one = (jax.random.normal(key_one, (3, 3, CHANNELS, CHANNELS), jnp.float32) * fan_scale).astype(jnp.bfloat16)
    w_two = (jax.random.normal(key_two, (3, 3, CHANNELS, CHANNELS), jnp.float32) * fan_scale).astype(jnp.bfloat16)
    return {"x_in": x_in, "a_pre": a_pre, "g_out": g_out, "w_one": w_one, "w_two": w_two}


def reference(x_in, a_pre, g_out, w_one, w_two):
    w_one_f = w_one.astype(jnp.float32)
    w_two_f = w_two.astype(jnp.float32)

    def conv_first(image_in):
        return conv_same(image_in, w_one_f)

    def conv_second(image_in):
        return conv_same(image_in, w_two_f)

    def one_image(packed):
        x_img, a_img, g_img = packed
        x_val = x_img[None].astype(jnp.float32)
        a_val = a_img[None].astype(jnp.float32)
        g_val = g_img[None].astype(jnp.float32)
        z_act = jax.nn.gelu(a_val, approximate=True).astype(jnp.bfloat16).astype(jnp.float32)
        d_z = jax.vjp(conv_second, z_act)[1](g_val)[0]
        d_w2 = tap_grads(jnp.pad(z_act, FRAME_PAD), g_val)
        d_a = (d_z * gelu_slope(a_val)).astype(jnp.bfloat16).astype(jnp.float32)
        conv_grad = jax.vjp(conv_first, x_val)[1](d_a)[0]
        d_w1 = tap_grads(jnp.pad(x_val, FRAME_PAD), d_a)
        d_x = (conv_grad + g_val).astype(jnp.bfloat16)
        return d_x[0], d_w1, d_w2

    d_x, w1_parts, w2_parts = lax.map(one_image, (x_in, a_pre, g_out))
    return d_x, jnp.sum(w1_parts, axis=0), jnp.sum(w2_parts, axis=0)
```

```python
import functools

import jax
import jax.numpy as jnp
from jax import lax
from jax.experimental import pallas as pl
from jax.experimental.pallas import tpu as pltpu
from jax.sharding import PartitionSpec as P

MESH = pl.DeviceIdType.MESH
F32 = jnp.float32
BF16 = jnp.bfloat16
IMGS = 2
ROWS = 48
COLS = 192
CH = 128
HALF = COLS // 2
G_ROWS = ROWS + 4
A_ROWS = ROWS + 2
TANH_SCALE = 0.7978845608028654
CUBE_COEF = 0.044715
A_STEP = 5
B_STEP = 8


def gelu_both(a_val):
    sq = a_val * a_val
    tanh_val = jnp.tanh(TANH_SCALE * (a_val + CUBE_COEF * sq * a_val))
    half = 0.5 * a_val
    plus = 1.0 + tanh_val
    slope = 0.5 * plus + half * (1.0 - tanh_val * tanh_val) * (TANH_SCALE + (TANH_SCALE * 3.0 * CUBE_COEF) * sq)
    return half * plus, slope


def halo_kernel(n_row, n_col, a_hbm, g_hbm, gn, gs, an, as_, rl, rr, cnw, cne, csw, cse,
                strip, wide, pack_l, pack_r, loc_sem, send_sem, recv_sem):
    row = lax.axis_index("row")
    col = lax.axis_index("col")
    has_n, has_s = row > 0, row < n_row - 1
    has_w, has_e = col > 0, col < n_col - 1
    dirs = {
        "n": (has_n, row - 1, col), "s": (has_s, row + 1, col),
        "w": (has_w, row, col - 1), "e": (has_e, row, col + 1),
        "nw": (has_n & has_w, row - 1, col - 1), "ne": (has_n & has_e, row - 1, col + 1),
        "sw": (has_s & has_w, row + 1, col - 1), "se": (has_s & has_e, row + 1, col + 1),
    }
    barrier = pltpu.get_barrier_semaphore()
    locals_ = []
    for k, (src, c0) in enumerate(((g_hbm, 0), (g_hbm, COLS - 16), (a_hbm, 0), (a_hbm, COLS - 16))):
        cp = pltpu.make_async_copy(src.at[:, :, pl.ds(c0, 16), :], strip.at[k], loc_sem.at[k])
        cp.start()
        locals_.append(cp)
    for ok, r, c in dirs.values():
        @pl.when(ok)
        def _(r=r, c=c):
            pl.semaphore_signal(barrier, inc=1, device_id=(c, r), device_id_type=MESH)
    for ok, refs in ((has_n, (gn, an)), (has_s, (gs, as_)), (has_w, (rl,)), (has_e, (rr,)),
                     (dirs["nw"][0], (cnw,)), (dirs["ne"][0], (cne,)), (dirs["sw"][0], (csw,)), (dirs["se"][0], (cse,))):
        @pl.when(jnp.logical_not(ok))
        def _(refs=refs):
            for ref in refs:
                ref[...] = jnp.zeros_like(ref)
    n_s, w_e = has_n.astype(jnp.int32) + has_s.astype(jnp.int32), has_w.astype(jnp.int32) + has_e.astype(jnp.int32)
    pl.semaphore_wait(barrier, n_s + w_e + n_s * w_e)

    def rcopy(k, src, dst, where):
        _, r, c = dirs[where]
        return pltpu.make_async_remote_copy(src_ref=src, dst_ref=dst, send_sem=send_sem.at[k], recv_sem=recv_sem.at[k],
                                            device_id=(c, r), device_id_type=MESH)

    copies = [
        ("s", "n", g_hbm.at[:, pl.ds(ROWS - 2, 2)], gn),
        ("n", "s", g_hbm.at[:, pl.ds(0, 2)], gs),
        ("s", "n", a_hbm.at[:, pl.ds(ROWS - 1, 1)], an),
        ("n", "s", a_hbm.at[:, pl.ds(0, 1)], as_),
        ("e", "w", pack_r, rl),
        ("w", "e", pack_l, rr),
        ("se", "nw", pack_r.at[:, :, pl.ds(32, 16)], cnw),
        ("sw", "ne", pack_l.at[:, :, pl.ds(32, 16)], cne),
        ("ne", "sw", pack_r.at[:, :, pl.ds(0, 16)], csw),
        ("nw", "se", pack_l.at[:, :, pl.ds(0, 16)], cse),
    ]

    def start(k):
        to, _, src, dst = copies[k]
        @pl.when(dirs[to][0])
        def _():
            rcopy(k, src, dst, to).start()

    for k in range(4):
        start(k)
    for k in range(4):
        locals_[k].wait()
        base = 0 if k % 2 == 0 else 8
        for m in range(IMGS):
            wide[...] = strip[k, m].astype(F32).reshape(ROWS * 16, CH)
            pack = pack_l if k % 2 == 0 else pack_r
            if k < 2:
                first = 0 if k == 0 else 14
                pack[m, 0] = wide[pl.ds(first, ROWS, stride=16), :].astype(BF16)
                pack[m, 1] = wide[pl.ds(first + 1, ROWS, stride=16), :].astype(BF16)
            else:
                pack[m, 2] = wide[pl.ds(0 if k == 2 else 15, ROWS, stride=16), :].astype(BF16)
    for k in range(4, 10):
        start(k)
    for k in range(10):
        to, frm, src, dst = copies[k]
        @pl.when(dirs[to][0])
        def _():
            rcopy(k, src, dst, to).wait_send()
        @pl.when(dirs[frm][0])
        def _():
            rcopy(k, src, dst, frm).wait_recv()


def halo(mesh_shape, a_tile, g_tile):
    vm = pl.BlockSpec(memory_space=pltpu.VMEM)
    outs = [((IMGS, 2, COLS, CH)), ((IMGS, 2, COLS, CH)), ((IMGS, 1, COLS, CH)), ((IMGS, 1, COLS, CH)),
            (IMGS, 3, ROWS, CH), (IMGS, 3, ROWS, CH)] + [(IMGS, 3, 16, CH)] * 4
    return pl.pallas_call(
        functools.partial(halo_kernel, mesh_shape["row"], mesh_shape["col"]),
        out_shape=[jax.ShapeDtypeStruct(s, BF16) for s in outs],
        in_specs=[pl.BlockSpec(memory_space=pl.ANY)] * 2,
        out_specs=[vm] * len(outs),
        scratch_shapes=[
            pltpu.VMEM((4, IMGS, ROWS, 16, CH), BF16),
            pltpu.VMEM((ROWS * 16, CH), F32),
            pltpu.VMEM((IMGS, 3, ROWS, CH), BF16),
            pltpu.VMEM((IMGS, 3, ROWS, CH), BF16),
            pltpu.SemaphoreType.DMA((4,)),
            pltpu.SemaphoreType.DMA((10,)),
            pltpu.SemaphoreType.DMA((10,)),
        ],
        compiler_params=pltpu.CompilerParams(collective_id=0, has_side_effects=True),
        name="halo",
    )(a_tile, g_tile)


def compute_kernel(n_row, n_col, x_hbm, a_hbm, g_hbm, gn, gs, an, as_, rl, rr, cnw, cne, csw, cse, w1, w2,
                   dx_hbm, dw,
                   g_buf, a_buf, x_buf, g4, d4, zp, band1, band2, w9, acc1, acc2, dz_ref,
                   s_g, s_a, s_e, s_o, gcol, acol, dcol, o_st,
                   in_sem, out_sem):
    row = lax.axis_index("row")
    col = lax.axis_index("col")
    loads = {}
    for m in range(IMGS):
        for j, (src, dst) in enumerate((
            (g_hbm.at[m], g_buf.at[m, pl.ds(2, ROWS)]), (gn.at[m], g_buf.at[m, pl.ds(0, 2)]), (gs.at[m], g_buf.at[m, pl.ds(ROWS + 2, 2)]),
            (a_hbm.at[m], a_buf.at[m, pl.ds(1, ROWS)]), (an.at[m], a_buf.at[m, pl.ds(0, 1)]), (as_.at[m], a_buf.at[m, pl.ds(ROWS + 1, 1)]),
            (x_hbm.at[m], x_buf.at[m]),
        )):
            loads[m, j] = pltpu.make_async_copy(src, dst, in_sem.at[m, j])
    for j in range(7):
        for m in range(IMGS):
            loads[m, j].start()

    for w, band in ((w1, band1), (w2, band2)):
        for dri in range(3):
            band[pl.ds(dri * 512 + 384, CH), pl.ds(0, CH)] = jnp.zeros((CH, CH), BF16)
            band[pl.ds(dri * 512, CH), pl.ds(CH, CH)] = jnp.zeros((CH, CH), BF16)
        for a in range(3):
            for c in range(3):
                tap = w[a, c].astype(F32).T.astype(BF16)
                dri = 2 - a
                band[pl.ds(dri * 512 + (2 - c) * CH, CH), pl.ds(0, CH)] = tap
                band[pl.ds(dri * 512 + (3 - c) * CH, CH), pl.ds(CH, CH)] = tap
                if w is w2:
                    w9[pl.ds((dri * 3 + 2 - c) * CH, CH), :] = tap
    acc1[...] = jnp.zeros_like(acc1)
    acc2[...] = jnp.zeros_like(acc2)

    for side, (mid, top, bot) in enumerate(((rl, cnw, csw), (rr, cne, cse))):
        for m in range(IMGS):
            for k in range(2):
                slot = k if side == 0 else k + 1
                gcol[side, m, slot, pl.ds(8, ROWS), :] = mid[m, k].astype(F32)
                gcol[side, m, slot, pl.ds(6, 2), :] = top[m, k].astype(F32)[14:16]
                gcol[side, m, slot, pl.ds(8 + ROWS, 2), :] = bot[m, k].astype(F32)[0:2]
            acol[side, m, pl.ds(8, ROWS), :] = mid[m, 2].astype(F32)
            acol[side, m, pl.ds(7, 1), :] = top[m, 2].astype(F32)[15:16]
            acol[side, m, pl.ds(8 + ROWS, 1), :] = bot[m, 2].astype(F32)[0:1]
    for m in range(IMGS):
        for j in range(3):
            loads[m, j].wait()
    for m in range(IMGS):
        for side in range(2):
            edge = g_buf[m, :, pl.ds(0 if side == 0 else COLS - 16, 16), :].astype(F32)
            s_g[pl.ds(0, G_ROWS * 16), :] = edge.reshape(G_ROWS * 16, CH)
            gcol[side, m, 2 if side == 0 else 0, pl.ds(6, G_ROWS), :] = s_g[pl.ds(0 if side == 0 else 15, G_ROWS, stride=16), :]
    for m in range(IMGS):
        for j in range(3, 7):
            loads[m, j].wait()
    for side in range(2):
        inside = (col > 0) if side == 0 else (col < n_col - 1)
        for m in range(IMGS):
            lhs = jnp.concatenate(
                [gcol[side, m, dci, pl.ds(6 + dri, 56), :].astype(BF16) for dri in range(3) for dci in range(3)], axis=1)
            dz_col = jnp.dot(lhs, w9[...], preferred_element_type=F32)
            _, slope = gelu_both(acol[side, m, pl.ds(7, 56), :])
            dcol[side, m] = jnp.where(inside, dz_col * slope, 0.0)

    def build_g4(n, carry):
        m, r0 = n // 13, (n % 13) * 4
        for t in range(4):
            base = t * 208
            s_g[pl.ds(base + 8, COLS), :] = g_buf[m, r0 + t].astype(F32)
            s_g[pl.ds(base + 7, 1), :] = gcol[0, m, 1, pl.ds(6 + r0 + t, 1), :]
            s_g[pl.ds(base + 8 + COLS, 1), :] = gcol[1, m, 1, pl.ds(6 + r0 + t, 1), :]
            at = pl.multiple_of((m * G_ROWS + r0 + t) * HALF, 32)
            for q in range(4):
                g4[pl.ds(at, HALF), pl.ds(q * CH, CH)] = s_g[pl.ds(base + 7 + q, HALF, stride=2), :].astype(BF16)
        return carry

    lax.fori_loop(0, 2 * 13, build_g4, 0)

    def conv_a(n):
        m, d0 = n // 10, (n % 10) * A_STEP
        lhs = jnp.concatenate(
            [g4[pl.ds(pl.multiple_of((m * G_ROWS + d0 + t) * HALF, 32), A_STEP * HALF), :] for t in range(3)], axis=1)
        return jnp.dot(lhs, band2[...], preferred_element_type=F32)

    dz_ref[...] = conv_a(0)

    def step_a(n, carry):
        m, d0 = n // 10, (n % 10) * A_STEP
        for t in range(A_STEP):
            base = t * COLS
            s_a[pl.ds(base, COLS), :] = a_buf[m, d0 + t].astype(F32)
            at = pl.multiple_of((m * A_ROWS + d0 + t) * HALF, 32)
            z_e, slope_e = gelu_both(s_a[pl.ds(base, HALF, stride=2), :])
            z_o, slope_o = gelu_both(s_a[pl.ds(base + 1, HALF, stride=2), :])
            zp[pl.ds(at, HALF), pl.ds(0, CH)] = z_e.astype(BF16)
            zp[pl.ds(at, HALF), pl.ds(CH, CH)] = z_o.astype(BF16)
            da_e = dz_ref[pl.ds(t * HALF, HALF), pl.ds(0, CH)] * slope_e
            da_o = dz_ref[pl.ds(t * HALF, HALF), pl.ds(CH, CH)] * slope_o
            s_e[t, pl.ds(8, HALF), :] = da_e
            s_o[t, pl.ds(8, HALF), :] = da_o
            s_o[t, pl.ds(7, 1), :] = dcol[0, m, pl.ds(d0 + t, 1), :]
            s_e[t, pl.ds(8 + HALF, 1), :] = dcol[1, m, pl.ds(d0 + t, 1), :]
            d4[pl.ds(at, HALF), pl.ds(0, CH)] = s_o[t, pl.ds(7, HALF), :].astype(BF16)
            d4[pl.ds(at, HALF), pl.ds(CH, CH)] = da_e.astype(BF16)
            d4[pl.ds(at, HALF), pl.ds(2 * CH, CH)] = da_o.astype(BF16)
            d4[pl.ds(at, HALF), pl.ds(3 * CH, CH)] = s_e[t, pl.ds(9, HALF), :].astype(BF16)
        dz_ref[...] = conv_a(jnp.minimum(n + 1, 19))
        return carry

    lax.fori_loop(0, 20, step_a, 0)
    for m in range(IMGS):
        for edge, ok in ((0, row > 0), (A_ROWS - 1, row < n_row - 1)):
            @pl.when(jnp.logical_not(ok))
            def _(m=m, edge=edge):
                d4[pl.ds((m * A_ROWS + edge) * HALF, HALF), :] = jnp.zeros((HALF, 4 * CH), BF16)

    def out_copy(n):
        m, r0 = n // 6, (n % 6) * B_STEP
        return pltpu.make_async_copy(o_st.at[n % 2], dx_hbm.at[m, pl.ds(r0, B_STEP)], out_sem.at[n % 2])

    def step_b(n, carry):
        m, r0 = n // 6, (n % 6) * B_STEP
        cnt = B_STEP * HALF
        z_chunk = zp[pl.ds(pl.multiple_of((m * A_ROWS + r0 + 1) * HALF, 32), cnt), :]
        g_win = jnp.concatenate(
            [g4[pl.ds(pl.multiple_of((m * G_ROWS + r0 + 1 + t) * HALF, 32), cnt), :] for t in range(3)], axis=1)
        acc2[...] += lax.dot_general(z_chunk, g_win, (((0,), (0,)), ((), ())), preferred_element_type=F32)
        xs = []
        for t in range(B_STEP):
            s_a[pl.ds(t * COLS, COLS), :] = x_buf[m, r0 + t].astype(F32)
        for t in range(B_STEP):
            xs.append(jnp.concatenate([s_a[pl.ds(t * COLS, HALF, stride=2), :].astype(BF16),
                                       s_a[pl.ds(t * COLS + 1, HALF, stride=2), :].astype(BF16)], axis=1))
        x_chunk = jnp.concatenate(xs, axis=0)
        d_win = jnp.concatenate(
            [d4[pl.ds(pl.multiple_of((m * A_ROWS + r0 + t) * HALF, 32), cnt), :] for t in range(3)], axis=1)
        acc1[...] += lax.dot_general(x_chunk, d_win, (((0,), (0,)), ((), ())), preferred_element_type=F32)
        dx = jnp.dot(d_win, band1[...], preferred_element_type=F32)
        g_own = g4[pl.ds(pl.multiple_of((m * G_ROWS + r0 + 2) * HALF, 32), cnt), pl.ds(CH, 2 * CH)].astype(F32)
        dx = dx + g_own

        @pl.when(n >= 2)
        def _():
            out_copy(n).wait()
        for t in range(B_STEP):
            s_g[pl.ds(t * COLS, HALF, stride=2), :] = dx[t * HALF:(t + 1) * HALF, :CH]
            s_g[pl.ds(t * COLS + 1, HALF, stride=2), :] = dx[t * HALF:(t + 1) * HALF, CH:]
        for t in range(B_STEP):
            o_st[n % 2, t] = s_g[pl.ds(t * COLS, COLS), :].astype(BF16)
        out_copy(n).start()
        return carry

    lax.fori_loop(0, 12, step_b, 0)
    for k, acc in enumerate((acc2, acc1)):
        for a in range(3):
            for c in range(3):
                at = (2 - a) * 512 + (2 - c) * CH
                dw[pl.ds((k * 9 + a * 3 + c) * CH, CH), :] = acc[pl.ds(0, CH), pl.ds(at, CH)] + acc[pl.ds(CH, CH), pl.ds(at + CH, CH)]
    out_copy(10).wait()
    out_copy(11).wait()


def compute(mesh_shape, x_tile, a_tile, g_tile, halos, w_one, w_two):
    vm = pl.BlockSpec(memory_space=pltpu.VMEM)
    hbm = pl.BlockSpec(memory_space=pl.ANY)
    return pl.pallas_call(
        functools.partial(compute_kernel, mesh_shape["row"], mesh_shape["col"]),
        out_shape=[jax.ShapeDtypeStruct((IMGS, ROWS, COLS, CH), BF16), jax.ShapeDtypeStruct((18 * CH, CH), F32)],
        in_specs=[hbm] * 7 + [vm] * 8,
        out_specs=[hbm, vm],
        scratch_shapes=[
            pltpu.VMEM((IMGS, G_ROWS, COLS, CH), BF16),
            pltpu.VMEM((IMGS, A_ROWS, COLS, CH), BF16),
            pltpu.VMEM((IMGS, ROWS, COLS, CH), BF16),
            pltpu.VMEM((IMGS * G_ROWS * HALF, 4 * CH), BF16),
            pltpu.VMEM((IMGS * A_ROWS * HALF, 4 * CH), BF16),
            pltpu.VMEM((IMGS * A_ROWS * HALF, 2 * CH), BF16),
            pltpu.VMEM((12 * CH, 2 * CH), BF16),
            pltpu.VMEM((12 * CH, 2 * CH), BF16),
            pltpu.VMEM((9 * CH, CH), BF16),
            pltpu.VMEM((2 * CH, 12 * CH), F32),
            pltpu.VMEM((2 * CH, 12 * CH), F32),
            pltpu.VMEM((A_STEP * HALF, 2 * CH), F32),
            pltpu.VMEM((B_STEP * COLS + 64, CH), F32),
            pltpu.VMEM((B_STEP * COLS, CH), F32),
            pltpu.VMEM((A_STEP, HALF + 16, CH), F32),
            pltpu.VMEM((A_STEP, HALF + 16, CH), F32),
            pltpu.VMEM((2, IMGS, 3, 72, CH), F32),
            pltpu.VMEM((2, IMGS, 72, CH), F32),
            pltpu.VMEM((2, IMGS, 56, CH), F32),
            pltpu.VMEM((2, B_STEP, COLS, CH), BF16),
            pltpu.SemaphoreType.DMA((IMGS, 7)),
            pltpu.SemaphoreType.DMA((2,)),
        ],
        compiler_params=pltpu.CompilerParams(vmem_limit_bytes=67043328),
        name="block_grads",
    )(x_tile, a_tile, g_tile, *halos, w_one, w_two)


CHAINS = ((0, 1024), (1024, 1280))


def sum_kernel(part, out1, out2, data, full, bufs0, bufs1, in_sem, send_sem, recv_sem):
    row, col = lax.axis_index("row"), lax.axis_index("col")
    x, core, z, y = row // 2, row % 2, col // 2, col % 2
    load = pltpu.make_async_copy(part, data, in_sem.at[0])
    load.start()
    x_peer = (col, 2 * (1 - x) + core)
    y_peer = (2 * z + 1 - y, row)
    core_peer = (col, 2 * x + 1 - core)
    z_peers = [(2 * ((z + t) % 4) + y, row) for t in (1, 2, 3)]
    barrier = pltpu.get_barrier_semaphore()
    for peer in (x_peer, y_peer, core_peer, *z_peers):
        pl.semaphore_signal(barrier, inc=1, device_id=peer, device_id_type=MESH)
    pl.semaphore_wait(barrier, 6)
    load.wait()
    first = (jnp.where(core == 0, col, y_peer[0]), jnp.where(core == 0, x_peer[1], row))
    second = (jnp.where(core == 0, y_peer[0], col), jnp.where(core == 0, row, x_peer[1]))
    bit1 = jnp.where(core == 0, x, y)
    bit2 = jnp.where(core == 0, y, x)
    sends = []

    def remote(src, dst, sem, peer):
        copy = pltpu.make_async_remote_copy(src_ref=src, dst_ref=dst, send_sem=send_sem.at[sem], recv_sem=recv_sem.at[sem],
                                            device_id=peer, device_id_type=MESH)
        return copy

    def rows(ref, at, count):
        return ref.at[pl.ds(pl.multiple_of(at, 8), count)]

    def chain(k):
        base, size = CHAINS[k]
        bufs = (bufs0, bufs1)[k]
        sem = 12 * k
        at = base
        buf_at = 0
        keep = base
        for stage, (bit, peer) in enumerate(((core, core_peer), (bit1, first), (bit2, second))):
            part_size = size >> (stage + 1)
            keep = at + bit * part_size
            copy = remote(rows(data, at + (1 - bit) * part_size, part_size), bufs.at[pl.ds(buf_at, part_size)], sem + stage, peer)
            copy.start()
            sends.append(copy)
            yield
            copy.wait_recv()
            mine = pl.ds(pl.multiple_of(keep, 8), part_size)
            data[mine, :] = data[mine, :] + bufs[pl.ds(buf_at, part_size), :]
            at = keep
            buf_at += part_size
        quarter = size // 32
        copies = []
        for t in (1, 2, 3):
            copy = remote(rows(data, at + ((z + t) % 4) * quarter, quarter), bufs.at[pl.ds(buf_at + (3 - t) * quarter, quarter)],
                          sem + 2 + t, z_peers[t - 1])
            copy.start()
            copies.append(copy)
        sends.extend(copies)
        yield
        for copy in copies:
            copy.wait_recv()
        mine = pl.ds(pl.multiple_of(at + z * quarter, 8), quarter)
        total = data[mine, :]
        for t in range(3):
            total = total + bufs[pl.ds(buf_at + t * quarter, quarter), :]
        full[mine, :] = total
        copies = []
        for t in (1, 2, 3):
            piece = rows(full, at + z * quarter, quarter)
            copy = remote(piece, piece, sem + 5 + t, z_peers[t - 1])
            copy.start()
            copies.append(copy)
        sends.extend(copies)
        yield
        for copy in copies:
            copy.wait_recv()
        for stage, (bit, peer) in ((2, (bit2, second)), (1, (bit1, first)), (0, (core, core_peer))):
            part_size = size >> (stage + 1)
            piece = rows(full, at, part_size)
            copy = remote(piece, piece, sem + 9 + stage, peer)
            copy.start()
            sends.append(copy)
            yield
            copy.wait_recv()
            at = at - bit * part_size

    running = [chain(0), chain(1)]
    while running:
        for one in list(running):
            try:
                next(one)
            except StopIteration:
                running.remove(one)
    for copy in sends:
        copy.wait_send()
    outs = [pltpu.make_async_copy(full.at[pl.ds(k * 9 * CH, 9 * CH)], (out2, out1)[k], in_sem.at[k]) for k in range(2)]
    for copy in outs:
        copy.start()
    for copy in outs:
        copy.wait()


def device_sum(part):
    hbm = pl.BlockSpec(memory_space=pl.ANY)
    return pl.pallas_call(
        sum_kernel,
        out_shape=[jax.ShapeDtypeStruct((9 * CH, CH), F32)] * 2,
        in_specs=[hbm],
        out_specs=[hbm] * 2,
        scratch_shapes=[
            pltpu.VMEM((18 * CH, CH), F32),
            pltpu.VMEM((18 * CH, CH), F32),
            pltpu.VMEM((1024, CH), F32),
            pltpu.VMEM((1280, CH), F32),
            pltpu.SemaphoreType.DMA((2,)),
            pltpu.SemaphoreType.DMA((24,)),
            pltpu.SemaphoreType.DMA((24,)),
        ],
        compiler_params=pltpu.CompilerParams(collective_id=1, has_side_effects=True),
        name="device_sum",
    )(part)


def solution(mesh):
    shape = dict(mesh.shape)

    def local_step(x_tile, a_tile, g_tile, w_one, w_two):
        halos = halo(shape, a_tile, g_tile)
        d_x, dw = compute(shape, x_tile, a_tile, g_tile, halos, w_one, w_two)
        d_w1, d_w2 = device_sum(dw)
        return d_x, d_w1.reshape(3, 3, CH, CH), d_w2.reshape(3, 3, CH, CH)

    tile_spec = P(None, "row", "col", None)
    return jax.shard_map(local_step, mesh=mesh, in_specs=(tile_spec, tile_spec, tile_spec, P(), P()), out_specs=(tile_spec, P(), P()), check_vma=False)
```

```python
import functools

import jax
import jax.numpy as jnp
from jax import lax
from jax.experimental import pallas as pl
from jax.experimental.pallas import tpu as pltpu
from jax.sharding import PartitionSpec as P

MESH = pl.DeviceIdType.MESH
F32 = jnp.float32
BF16 = jnp.bfloat16
IMGS = 2
ROWS = 48
COLS = 192
CH = 128
HALF = COLS // 2
G_ROWS = ROWS + 4
A_ROWS = ROWS + 2
TANH_SCALE = 0.7978845608028654
CUBE_COEF = 0.044715
STEP = 8
TILE = 32
BY_ROWS = (((0,), (0,)), ((), ()))
CHUNKS = IMGS * ROWS // STEP
PER = ROWS // STEP
CHAINS = ((0, 1024), (1024, 768), (1792, 512))
CHAIN_SEMS = 14
TAP_ROWS = 3 * CH
LO, HI = pl.ds(0, CH), pl.ds(CH, CH)
WIN = 4 * CH


def gelu_both(a_val):
    sq = a_val * a_val
    tanh_val = jnp.tanh(a_val * (TANH_SCALE + (TANH_SCALE * CUBE_COEF) * sq))
    half_plus = 0.5 + 0.5 * tanh_val
    inner = (0.5 * TANH_SCALE) + (1.5 * TANH_SCALE * CUBE_COEF) * sq
    return a_val * half_plus, half_plus + ((1.0 - tanh_val * tanh_val) * a_val) * inner


def matmul_halves(lhs, rhs, out):
    count = lhs.shape[0] // 2
    for k in range(2):
        out[pl.ds(k * count, count), :] = jnp.dot(lhs[k * count:(k + 1) * count], rhs, preferred_element_type=F32)


def make_chain(base, size, first_sem, data, full, bufs, send_sem, recv_sem, place, last=6):
    core, quadrant, z, core_peer, xy_peers, z_peers = place
    half, eighth, quarter = size // 2, size // 8, size // 32
    mine0 = base + core * half
    away0 = base + half - core * half
    mine1 = mine0 + quadrant * eighth
    away1 = [mine0 + (3 - quadrant) * eighth, mine0 + (quadrant + 1 - 2 * (quadrant % 2)) * eighth,
             mine0 + (quadrant + 2 - 4 * (quadrant // 2)) * eighth]
    mine2 = mine1 + z * quarter
    away2 = [mine1 + ((z + 1 + t) % 4) * quarter for t in range(3)]
    slots1 = [half + t * eighth for t in range(3)]
    slots2 = [half + 3 * eighth + t * quarter for t in range(3)]

    def rows(ref, start, count):
        return ref.at[pl.ds(pl.multiple_of(start, 8), count)]

    def remote(src, dst, sem, peer):
        return pltpu.make_async_remote_copy(src_ref=src, dst_ref=dst, send_sem=send_sem.at[first_sem + sem],
                                            recv_sem=recv_sem.at[first_sem + sem], device_id=peer, device_id_type=MESH)

    def same(start, count, sem, peer):
        return remote(rows(full, start, count), rows(full, start, count), sem, peer)

    stages = [
        lambda: [remote(rows(data, away0, half), rows(bufs, 0, half), 0, core_peer)],
        lambda: [remote(rows(data, away1[t], eighth), rows(bufs, slots1[t], eighth), 1 + t, xy_peers[t]) for t in range(3)],
        lambda: [remote(rows(data, away2[t], quarter), rows(bufs, slots2[t], quarter), 4 + t, z_peers[t]) for t in range(3)],
        lambda: [same(mine2, quarter, 7 + t, z_peers[t]) for t in range(3)],
        lambda: [same(mine1, eighth, 10 + t, xy_peers[t]) for t in range(3)],
        lambda: [same(mine0, half, 13, core_peer)],
    ]
    adds = [(data, mine0, half, [0]), (data, mine1, eighth, slots1), (full, mine2, quarter, slots2)]

    def step(k):
        if k > 0:
            for copy in stages[k - 1]():
                copy.wait_recv()
        if 0 < k <= len(adds):
            dst, start, count, slots = adds[k - 1]
            spot = pl.ds(pl.multiple_of(start, 8), count)
            total = data[spot, :]
            for slot in slots:
                total = total + bufs[pl.ds(slot, count), :]
            dst[spot, :] = total
        if k < last:
            for copy in stages[k]():
                copy.start()
        else:
            for stage in stages[:last]:
                for copy in stage():
                    copy.wait_send()

    return step


def block_kernel(n_row, n_col, x_hbm, a_hbm, g_hbm, w1, w2, dx_hbm, out,
                 g_buf, a_buf, x_buf, g4, d4, band1, band2, w9, acc1, acc2, dz0, dz1, zb0, zb1, xp,
                 s_g, s_a, s_e, s_o, gcol, acol, dcol,
                 strip, pack_l, pack_r, rl, rr, corners, data, full, bufs0, bufs1, bufs2,
                 in_sem, out_sem, loc_sem, hsend_sem, hrecv_sem, send_sem, recv_sem):
    row, col = lax.axis_index("row"), lax.axis_index("col")
    x, core, z, y = row // 2, row % 2, col // 2, col % 2
    x_peer, y_peer = (col, 2 * (1 - x) + core), (2 * z + 1 - y, row)
    core_peer = (col, 2 * x + 1 - core)
    z_peers = [(2 * ((z + t) % 4) + y, row) for t in (1, 2, 3)]
    xy_peers = [(y_peer[0], x_peer[1]), y_peer, x_peer]
    place = (core, 2 * x + y, z, core_peer, xy_peers, z_peers)
    chain0, chain1, chain2 = (make_chain(*rows, CHAIN_SEMS * k, data, full, bufs, send_sem, recv_sem, place)
                              for k, (rows, bufs) in enumerate(zip(CHAINS, (bufs0, bufs1, bufs2))))

    has_n, has_s, has_w, has_e = row > 0, row < n_row - 1, col > 0, col < n_col - 1
    dirs = {
        "n": (has_n, row - 1, col), "s": (has_s, row + 1, col),
        "w": (has_w, row, col - 1), "e": (has_e, row, col + 1),
        "nw": (has_n & has_w, row - 1, col - 1), "ne": (has_n & has_e, row - 1, col + 1),
        "sw": (has_s & has_w, row + 1, col - 1), "se": (has_s & has_e, row + 1, col + 1),
    }
    barrier = pltpu.get_barrier_semaphore()
    for ok, r, c in dirs.values():
        @pl.when(ok)
        def _(r=r, c=c):
            pl.semaphore_signal(barrier, inc=1, device_id=(c, r), device_id_type=MESH)
    for peer in (core_peer, *xy_peers, *z_peers):
        pl.semaphore_signal(barrier, inc=1, device_id=peer, device_id_type=MESH)
    strips = [pltpu.make_async_copy(src.at[:, :, pl.ds(c0, 16), :], strip.at[k], loc_sem.at[k])
              for k, (src, c0) in enumerate(((g_hbm, 0), (g_hbm, COLS - 16), (a_hbm, 0), (a_hbm, COLS - 16)))]
    for cp in strips:
        cp.start()
    loads = [[pltpu.make_async_copy(src.at[m], dst, in_sem.at[m, j]) for j, (src, dst) in enumerate((
        (g_hbm, g_buf.at[m, pl.ds(2, ROWS)]), (a_hbm, a_buf.at[m, pl.ds(1, ROWS)]), (x_hbm, x_buf.at[m])))] for m in range(IMGS)]
    for j in range(3):
        for m in range(IMGS):
            loads[m][j].start()
    for ok, views in ((has_n, [g_buf.at[:, pl.ds(0, 2)], a_buf.at[:, pl.ds(0, 1)]]),
                      (has_s, [g_buf.at[:, pl.ds(ROWS + 2, 2)], a_buf.at[:, pl.ds(ROWS + 1, 1)]]),
                      (has_w, [rl]), (has_e, [rr]),
                      (dirs["nw"][0], [corners.at[0]]), (dirs["ne"][0], [corners.at[1]]),
                      (dirs["sw"][0], [corners.at[2]]), (dirs["se"][0], [corners.at[3]])):
        @pl.when(jnp.logical_not(ok))
        def _(views=views):
            for view in views:
                view[...] = jnp.zeros(view.shape, BF16)
    n_s, w_e = has_n.astype(jnp.int32) + has_s.astype(jnp.int32), has_w.astype(jnp.int32) + has_e.astype(jnp.int32)
    pl.semaphore_wait(barrier, n_s + w_e + n_s * w_e + 7)

    copies = [
        ("s", "n", g_hbm.at[:, pl.ds(ROWS - 2, 2)], g_buf.at[:, pl.ds(0, 2)]),
        ("n", "s", g_hbm.at[:, pl.ds(0, 2)], g_buf.at[:, pl.ds(ROWS + 2, 2)]),
        ("s", "n", a_hbm.at[:, pl.ds(ROWS - 1, 1)], a_buf.at[:, pl.ds(0, 1)]),
        ("n", "s", a_hbm.at[:, pl.ds(0, 1)], a_buf.at[:, pl.ds(ROWS + 1, 1)]),
        ("e", "w", pack_r, rl),
        ("w", "e", pack_l, rr),
        ("se", "nw", pack_r.at[:, :, pl.ds(32, 16)], corners.at[0]),
        ("sw", "ne", pack_l.at[:, :, pl.ds(32, 16)], corners.at[1]),
        ("ne", "sw", pack_r.at[:, :, pl.ds(0, 16)], corners.at[2]),
        ("nw", "se", pack_l.at[:, :, pl.ds(0, 16)], corners.at[3]),
    ]

    def rcopy(k, where):
        _, r, c = dirs[where]
        return pltpu.make_async_remote_copy(src_ref=copies[k][2], dst_ref=copies[k][3], send_sem=hsend_sem.at[k],
                                            recv_sem=hrecv_sem.at[k], device_id=(c, r), device_id_type=MESH)

    def start_halo(k):
        @pl.when(dirs[copies[k][0]][0])
        def _():
            rcopy(k, copies[k][0]).start()

    for k in range(4):
        start_halo(k)
    for k in range(4):
        strips[k].wait()
        pack = pack_l if k % 2 == 0 else pack_r
        for m in range(IMGS):
            s_g[pl.ds(0, ROWS * 16), :] = strip[k, m].astype(F32).reshape(ROWS * 16, CH)
            for slot, first_col in (((0, 0 if k == 0 else 14), (1, 1 if k == 0 else 15)) if k < 2 else ((2, 0 if k == 2 else 15),)):
                pack[m, slot] = s_g[pl.ds(first_col, ROWS, stride=16), :].astype(BF16)
    for k in range(4, 10):
        start_halo(k)

    for w, band in ((w1, band1), (w2, band2)):
        for dri in range(3):
            band[pl.ds(dri * 512 + 384, CH), LO] = jnp.zeros((CH, CH), BF16)
            band[pl.ds(dri * 512, CH), HI] = jnp.zeros((CH, CH), BF16)
        for a in range(3):
            for c in range(3):
                tap = w[a, c].astype(F32).T.astype(BF16)
                dri = 2 - a
                band[pl.ds(dri * 512 + (2 - c) * CH, CH), LO] = tap
                band[pl.ds(dri * 512 + (3 - c) * CH, CH), HI] = tap
                if w is w2:
                    w9[pl.ds((dri * 3 + 2 - c) * CH, CH), :] = tap
    acc1[...] = jnp.zeros_like(acc1)
    acc2[...] = jnp.zeros_like(acc2)
    zb1[...] = jnp.zeros_like(zb1)

    def window_row(m, r, t):
        base = t * 208
        s_g[pl.ds(base + 8, COLS), :] = g_buf[m, r].astype(F32)
        at = pl.multiple_of((m * G_ROWS + r) * HALF, TILE)
        for q in range(4):
            g4[pl.ds(at, HALF), pl.ds(q * CH, CH)] = s_g[pl.ds(base + 7 + q, HALF, stride=2), :].astype(BF16)

    def build_g4(n, carry):
        for t in range(4):
            window_row(n // 12, 2 + (n % 12) * 4 + t, t)
        return carry

    def prep_x(n, carry):
        m, r0 = n // PER, (n % PER) * STEP
        at = pl.multiple_of(n * STEP * HALF, TILE)
        for t in range(STEP):
            s_a[pl.ds(t * COLS, COLS), :] = x_buf[m, r0 + t].astype(F32)
            for q in range(2):
                xp[pl.ds(at + t * HALF, HALF), pl.ds(q * CH, CH)] = s_a[pl.ds(t * COLS + q, HALF, stride=2), :].astype(BF16)
        return carry

    s_g[...] = jnp.zeros_like(s_g)
    for m in range(IMGS):
        loads[m][0].wait()
    lax.fori_loop(0, 24, build_g4, 0)
    for m in range(IMGS):
        loads[m][2].wait()
    lax.fori_loop(0, CHUNKS, prep_x, 0)

    for k in range(10):
        to, frm = copies[k][:2]
        @pl.when(dirs[to][0])
        def _():
            rcopy(k, to).wait_send()
        @pl.when(dirs[frm][0])
        def _():
            rcopy(k, frm).wait_recv()

    for side, (beside, top, bot) in enumerate(((rl, 0, 2), (rr, 1, 3))):
        for m in range(IMGS):
            for k in range(2):
                slot = k if side == 0 else k + 1
                gcol[side, m, slot, pl.ds(8, ROWS), :] = beside[m, k].astype(F32)
                gcol[side, m, slot, pl.ds(6, 2), :] = corners[top, m, k].astype(F32)[14:16]
                gcol[side, m, slot, pl.ds(8 + ROWS, 2), :] = corners[bot, m, k].astype(F32)[0:2]
            acol[side, m, pl.ds(8, ROWS), :] = beside[m, 2].astype(F32)
            acol[side, m, pl.ds(7, 1), :] = corners[top, m, 2].astype(F32)[15:16]
            acol[side, m, pl.ds(8 + ROWS, 1), :] = corners[bot, m, 2].astype(F32)[0:1]
    for m in range(IMGS):
        for side in range(2):
            edge = g_buf[m, :, pl.ds(0 if side == 0 else COLS - 16, 16), :].astype(F32)
            s_g[pl.ds(0, G_ROWS * 16), :] = edge.reshape(G_ROWS * 16, CH)
            gcol[side, m, 2 if side == 0 else 0, pl.ds(6, G_ROWS), :] = s_g[pl.ds(0 if side == 0 else 15, G_ROWS, stride=16), :]
    lhs = jnp.concatenate([jnp.concatenate(
        [gcol[side, m, dci, pl.ds(6 + dri, 64), :].astype(BF16) for dri in range(3) for dci in range(3)], axis=1)
        for side in range(2) for m in range(IMGS)], axis=0)
    dz_col = jnp.dot(lhs, w9[...], preferred_element_type=F32)
    for side, inside in ((0, has_w), (1, has_e)):
        for m in range(IMGS):
            _, slope = gelu_both(acol[side, m, pl.ds(7, 64), :])
            first_row = (side * IMGS + m) * 64
            dcol[side, m] = jnp.where(inside, dz_col[first_row:first_row + 64] * slope, 0.0)

    for m in range(IMGS):
        for t, r in enumerate((0, 1, G_ROWS - 2, G_ROWS - 1)):
            window_row(m, r, t)
    line = lax.broadcasted_iota(jnp.int32, (16, CH), 0)

    def patch(n, carry):
        for t in range(4):
            for m in range(IMGS):
                r = n * 4 + t
                at = pl.multiple_of((m * G_ROWS + r) * HALF, TILE)
                for side, where, q, hit in ((0, at, 0, 0), (1, at + HALF - 16, 3, 15)):
                    spot = (pl.ds(pl.multiple_of(where, 16), 16), pl.ds(q * CH, CH))
                    new = jnp.broadcast_to(gcol[side, m, 1, pl.ds(6 + r, 1), :], (16, CH))
                    g4[spot] = jnp.where(line == hit, new, g4[spot].astype(F32)).astype(BF16)
        return carry

    lax.fori_loop(0, 13, patch, 0)
    for m in range(IMGS):
        loads[m][1].wait()

    def g_rows(m, r, count):
        return g4[pl.ds(pl.multiple_of((m * G_ROWS + r) * HALF, TILE), count * HALF), :]

    def d_rows(m, r, count):
        return d4[pl.ds(pl.multiple_of((m * A_ROWS + r) * HALF, TILE), count * HALF), :]

    def one_row(m, d, t, dz, zb):
        base = t * COLS
        s_a[pl.ds(base, COLS), :] = a_buf[m, d].astype(F32)
        at = pl.multiple_of((m * A_ROWS + d) * HALF, TILE)
        z_e, slope_e = gelu_both(s_a[pl.ds(base, HALF, stride=2), :])
        z_o, slope_o = gelu_both(s_a[pl.ds(base + 1, HALF, stride=2), :])
        if zb is not None:
            zb[pl.ds(t * HALF, HALF), LO] = z_e.astype(BF16)
            zb[pl.ds(t * HALF, HALF), HI] = z_o.astype(BF16)
        da_e = dz[pl.ds(t * HALF, HALF), LO] * slope_e
        da_o = dz[pl.ds(t * HALF, HALF), HI] * slope_o
        s_e[t, pl.ds(8, HALF), :] = da_e
        s_o[t, pl.ds(8, HALF), :] = da_o
        s_o[t, pl.ds(7, 1), :] = dcol[0, m, pl.ds(d, 1), :]
        s_e[t, pl.ds(8 + HALF, 1), :] = dcol[1, m, pl.ds(d, 1), :]
        d4[pl.ds(at, HALF), LO] = s_o[t, pl.ds(7, HALF), :].astype(BF16)
        d4[pl.ds(at, HALF), HI] = da_e.astype(BF16)
        d4[pl.ds(at, HALF), pl.ds(2 * CH, CH)] = da_o.astype(BF16)
        d4[pl.ds(at, HALF), pl.ds(3 * CH, CH)] = s_e[t, pl.ds(9, HALF), :].astype(BF16)

    frame = [(m, d) for m in range(IMGS) for d in (0, A_ROWS - 1)]
    lhs = jnp.concatenate([jnp.concatenate([g_rows(m, d + t, 1) for t in range(3)], axis=1) for m, d in frame], axis=0)
    matmul_halves(lhs, band2[...], dz0)
    for t, (m, d) in enumerate(frame):
        one_row(m, d, t, dz0, None)
    for edge, ok in ((0, has_n), (A_ROWS - 1, has_s)):
        @pl.when(jnp.logical_not(ok))
        def _(edge=edge):
            for m in range(IMGS):
                d4[pl.ds((m * A_ROWS + edge) * HALF, HALF), :] = jnp.zeros((HALF, 4 * CH), BF16)

    def conv_a(n, out):
        m, r0 = n // PER, (n % PER) * STEP
        lhs = jnp.concatenate([g_rows(m, r0 + 1 + t, STEP) for t in range(3)], axis=1)
        matmul_halves(lhs, band2[...], out)

    def grad2(n, zb):
        m, r0 = n // PER, (n % PER) * STEP
        win = jnp.concatenate([g_rows(m, r0 + 1 + t, STEP) for t in range(3)], axis=1)
        acc2[...] += lax.dot_general(zb[...], win, BY_ROWS, preferred_element_type=F32)

    conv_a(0, dz0)

    def step_a(i, carry):
        for n, dz, dz_next, zb, zb_last in ((2 * i, dz0, dz1, zb0, zb1), (2 * i + 1, dz1, dz0, zb1, zb0)):
            m, r0 = n // PER, (n % PER) * STEP
            conv_a(jnp.minimum(n + 1, CHUNKS - 1), dz_next)
            grad2(jnp.maximum(n - 1, 0), zb_last)
            for t in range(STEP):
                one_row(m, r0 + 1 + t, t, dz, zb)
        return carry

    lax.fori_loop(0, CHUNKS // 2, step_a, 0)
    grad2(CHUNKS - 1, zb1)

    def fold(acc, a, at):
        for c in range(3):
            left, top = (2 - a) * WIN + (2 - c) * CH, at + c * CH
            data[pl.ds(top, CH), :] = acc[LO, pl.ds(left, CH)] + acc[HI, pl.ds(left + CH, CH)]

    for a in range(3):
        fold(acc2, a, a * TAP_ROWS)
    chain0(0)

    def at_steps(i, table):
        for when, chain, k in table:
            def run(_, carry, chain=chain, k=k):
                chain(k)
                return carry

            lax.fori_loop(0, (i == when).astype(jnp.int32), run, 0)

    def grad1(i, dris):
        m, r0 = i // 3, (i % 3) * 2 * STEP
        win = jnp.concatenate([d_rows(m, r0 + t, 2 * STEP) for t in dris], axis=1)
        x_rows = xp[pl.ds(pl.multiple_of(i * 2 * STEP * HALF, TILE), 2 * STEP * HALF), :]
        spot = pl.ds(dris[0] * WIN, len(dris) * WIN)
        acc1[:, spot] += lax.dot_general(x_rows, win, BY_ROWS, preferred_element_type=F32)

    def step_b(i, carry):
        at_steps(i, ((2, chain0, 1),))
        grad1(i, (0, 1))
        return carry

    def step_b2(i, carry):
        at_steps(i, ((1, chain0, 2), (3, chain1, 1)))
        grad1(i, (2,))
        return carry

    lax.fori_loop(0, CHUNKS // 2, step_b, 0)
    fold(acc1, 1, 3 * TAP_ROWS)
    fold(acc1, 2, 4 * TAP_ROWS)
    chain1(0)
    lax.fori_loop(0, CHUNKS // 2, step_b2, 0)
    fold(acc1, 0, 5 * TAP_ROWS)
    chain2(0)

    def conv_x(n, out):
        m, r0 = n // PER, (n % PER) * STEP
        win = jnp.concatenate([d_rows(m, r0 + t, STEP) for t in range(3)], axis=1)
        matmul_halves(win, band1[...], out)

    def out_copy(n):
        rows = pl.ds((n % PER) * STEP, STEP)
        return pltpu.make_async_copy(x_buf.at[n // PER, rows], dx_hbm.at[n // PER, rows], out_sem.at[n])

    def finish(n, dz):
        m, r0 = n // PER, (n % PER) * STEP
        own = g4[pl.ds(pl.multiple_of((m * G_ROWS + r0 + 2) * HALF, TILE), STEP * HALF), pl.ds(CH, 2 * CH)].astype(F32)
        for t in range(STEP):
            part = dz[pl.ds(t * HALF, HALF), :] + own[t * HALF:(t + 1) * HALF]
            for q in range(2):
                s_a[pl.ds(t * COLS + q, HALF, stride=2), :] = part[:, q * CH:(q + 1) * CH]
            x_buf[m, r0 + t] = s_a[pl.ds(t * COLS, COLS), :].astype(BF16)
        out_copy(n).start()

    conv_x(0, dz0)

    def step_c(i, carry):
        at_steps(i, ((1, chain2, 1), (3, chain2, 2), (5, chain2, 3)))
        conv_x(2 * i + 1, dz1)
        finish(2 * i, dz0)
        at_steps(i, ((0, chain0, 3), (1, chain1, 2), (2, chain0, 4), (3, chain1, 3), (4, chain0, 5), (5, chain1, 4)))
        conv_x(jnp.minimum(2 * i + 2, CHUNKS - 1), dz0)
        finish(2 * i + 1, dz1)
        return carry

    lax.fori_loop(0, CHUNKS // 2, step_c, 0)
    for chain, k in ((chain0, 6), (chain1, 5), (chain2, 4), (chain1, 6), (chain2, 5), (chain2, 6)):
        chain(k)
    result = pltpu.make_async_copy(full, out, loc_sem.at[0])
    result.start()
    for n in range(CHUNKS):
        out_copy(n).wait()
    result.wait()


def place_kernel(dx_in, dw_in, dx_out, dw1_out, dw2_out, dx_buf, dw_buf, in_sem, out_sem):
    halves = ROWS // 2
    pieces = [(dx_in.at[k // 2, pl.ds(k % 2 * halves, halves)], dx_buf.at[k // 2, pl.ds(k % 2 * halves, halves)],
               dx_out.at[k // 2, pl.ds(k % 2 * halves, halves)]) for k in range(4)]
    for k, (dst, at) in enumerate(((dw2_out, 0), (dw1_out, 5), (dw1_out, 3))):
        count = (3, 1, 2)[k] * TAP_ROWS
        rows = pl.ds(at * TAP_ROWS, count)
        pieces.append((dw_in.at[rows], dw_buf.at[rows], dst.at[pl.ds((0, 0, TAP_ROWS)[k], count)]))
    loads = [pltpu.make_async_copy(src, mid, in_sem.at[k]) for k, (src, mid, _) in enumerate(pieces)]
    stores = [pltpu.make_async_copy(mid, dst, out_sem.at[k]) for k, (_, mid, dst) in enumerate(pieces)]
    for copy in loads:
        copy.start()
    for load, store in zip(loads, stores):
        load.wait()
        store.start()
    for store in stores:
        store.wait()


def place_results(d_x, dw):
    hbm = pl.BlockSpec(memory_space=pl.ANY)
    taps = jax.ShapeDtypeStruct((9 * CH, CH), F32)
    return pl.pallas_call(
        place_kernel,
        out_shape=[jax.ShapeDtypeStruct(d_x.shape, BF16), taps, taps],
        in_specs=[hbm] * 2,
        out_specs=[hbm] * 3,
        scratch_shapes=[pltpu.VMEM(d_x.shape, BF16), pltpu.VMEM(dw.shape, F32), pltpu.SemaphoreType.DMA((7,)), pltpu.SemaphoreType.DMA((7,))],
        name="place_results",
    )(d_x, dw)


def block_grads(mesh_shape, x_tile, a_tile, g_tile, w_one, w_two):
    vm = pl.BlockSpec(memory_space=pltpu.VMEM)
    hbm = pl.BlockSpec(memory_space=pl.ANY)
    half, pair = STEP * HALF, 2 * CH
    padded, cols = (STEP, HALF + 16, CH), (IMGS, 3, ROWS, CH)
    return pl.pallas_call(
        functools.partial(block_kernel, mesh_shape["row"], mesh_shape["col"]),
        out_shape=[jax.ShapeDtypeStruct((IMGS, ROWS, COLS, CH), BF16), jax.ShapeDtypeStruct((18 * CH, CH), F32)],
        in_specs=[hbm] * 3 + [vm] * 2,
        out_specs=[hbm] * 2,
        scratch_shapes=[pltpu.VMEM(shape, BF16) for shape in (
            (IMGS, G_ROWS, COLS, CH), (IMGS, A_ROWS, COLS, CH), (IMGS, ROWS, COLS, CH),
            (IMGS * G_ROWS * HALF, WIN), (IMGS * A_ROWS * HALF, WIN), (3 * WIN, pair), (3 * WIN, pair), (9 * CH, CH))
        ] + [pltpu.VMEM(shape, F32) for shape in ((pair, 3 * WIN), (pair, 3 * WIN), (half, pair), (half, pair))
        ] + [pltpu.VMEM(shape, BF16) for shape in ((half, pair), (half, pair), (CHUNKS * half, pair))
        ] + [pltpu.VMEM(shape, F32) for shape in (
            (4 * 208 + 16, CH), (STEP * COLS, CH), padded, padded, (2, IMGS, 3, 72, CH), (2, IMGS, 72, CH), (2, IMGS, 64, CH))
        ] + [pltpu.VMEM(shape, BF16) for shape in ((4, IMGS, ROWS, 16, CH), cols, cols, cols, cols, (4, IMGS, 3, 16, CH))
        ] + [pltpu.VMEM(shape, F32) for shape in ((18 * CH, CH), (18 * CH, CH), *((size, CH) for _, size in CHAINS))
        ] + [pltpu.SemaphoreType.DMA(shape) for shape in ((IMGS, 3), (CHUNKS,), (4,), (10,), (10,), (3 * CHAIN_SEMS,), (3 * CHAIN_SEMS,))],
        compiler_params=pltpu.CompilerParams(collective_id=0, has_side_effects=True, vmem_limit_bytes=67043328),
        name="block_grads",
    )(x_tile, a_tile, g_tile, w_one, w_two)


def solution(mesh):
    shape = dict(mesh.shape)

    def local_step(x_tile, a_tile, g_tile, w_one, w_two):
        d_x, dw = block_grads(shape, x_tile, a_tile, g_tile, w_one, w_two)
        d_x, d_w1, d_w2 = place_results(d_x, dw)
        return d_x, d_w1.reshape(w_one.shape), d_w2.reshape(w_two.shape)

    tile_spec = P(None, "row", "col", None)
    return jax.shard_map(local_step, mesh=mesh, in_specs=(tile_spec, tile_spec, tile_spec, P(), P()), out_specs=(tile_spec, P(), P()), check_vma=False)
```

```python
import functools

import jax
import jax.numpy as jnp
from jax import lax
from jax.experimental import pallas as pl
from jax.experimental.pallas import tpu as pltpu
from jax.sharding import PartitionSpec as P

MESH = pl.DeviceIdType.MESH
F32 = jnp.float32
BF16 = jnp.bfloat16
IMGS = 2
ROWS = 48
COLS = 192
CH = 128
HALF = COLS // 2
G_ROWS = ROWS + 4
A_ROWS = ROWS + 2
TANH_SCALE = 0.7978845608028654
CUBE_COEF = 0.044715
STEP = 8
TILE = 32
BY_ROWS = (((0,), (0,)), ((), ()))
CHUNKS = IMGS * ROWS // STEP
PER = ROWS // STEP
CHAINS = ((0, 1024), (1024, 768), (1792, 512))
A_STEP = 6
A_PER = ROWS // A_STEP
A_UNROLL = 2
TURNS = 1
CHAIN_SEMS = 14
BLOCK_BYTES = 61145088
PLACE_BYTES = 1048576
TAP_ROWS = 3 * CH
LO, HI = pl.ds(0, CH), pl.ds(CH, CH)
WIN = 4 * CH


def gelu_both(a_val):
    sq = a_val * a_val
    tanh_val = jnp.tanh(a_val * (TANH_SCALE + (TANH_SCALE * CUBE_COEF) * sq))
    half_plus = 0.5 + 0.5 * tanh_val
    inner = (0.5 * TANH_SCALE) + (1.5 * TANH_SCALE * CUBE_COEF) * sq
    return a_val * half_plus, half_plus + ((1.0 - tanh_val * tanh_val) * a_val) * inner


def matmul_halves(lhs, rhs, out):
    count = lhs.shape[0] // 2
    for k in range(2):
        out[pl.ds(k * count, count), :] = jnp.dot(lhs[k * count:(k + 1) * count], rhs, preferred_element_type=F32)


def make_chain(base, size, first_sem, data, full, bufs, send_sem, recv_sem, place, last=6):
    core, quadrant, z, core_peer, xy_peers, z_peers = place
    half, eighth, quarter = size // 2, size // 8, size // 32
    mine0 = base + core * half
    away0 = base + half - core * half
    mine1 = mine0 + quadrant * eighth
    away1 = [mine0 + (3 - quadrant) * eighth, mine0 + (quadrant + 1 - 2 * (quadrant % 2)) * eighth,
             mine0 + (quadrant + 2 - 4 * (quadrant // 2)) * eighth]
    mine2 = mine1 + z * quarter
    away2 = [mine1 + ((z + 1 + t) % 4) * quarter for t in range(3)]
    slots1 = [half + t * eighth for t in range(3)]
    slots2 = [half + 3 * eighth + t * quarter for t in range(3)]

    def rows(ref, start, count):
        return ref.at[pl.ds(pl.multiple_of(start, 8), count)]

    def remote(src, dst, sem, peer):
        return pltpu.make_async_remote_copy(src_ref=src, dst_ref=dst, send_sem=send_sem.at[first_sem + sem],
                                            recv_sem=recv_sem.at[first_sem + sem], device_id=peer, device_id_type=MESH)

    def same(start, count, sem, peer):
        return remote(rows(full, start, count), rows(full, start, count), sem, peer)

    stages = [
        lambda: [remote(rows(data, away0, half), rows(bufs, 0, half), 0, core_peer)],
        lambda: [remote(rows(data, away1[t], eighth), rows(bufs, slots1[t], eighth), 1 + t, xy_peers[t]) for t in range(3)],
        lambda: [remote(rows(data, away2[t], quarter), rows(bufs, slots2[t], quarter), 4 + t, z_peers[t]) for t in range(3)],
        lambda: [same(mine2, quarter, 7 + t, z_peers[t]) for t in range(3)],
        lambda: [same(mine1, eighth, 10 + t, xy_peers[t]) for t in range(3)],
        lambda: [same(mine0, half, 13, core_peer)],
    ]
    adds = [(data, mine0, half, [0]), (data, mine1, eighth, slots1), (full, mine2, quarter, slots2)]

    def step(k):
        if k > 0:
            for copy in stages[k - 1]():
                copy.wait_recv()
        if 0 < k <= len(adds):
            dst, start, count, slots = adds[k - 1]
            spot = pl.ds(pl.multiple_of(start, 8), count)
            total = data[spot, :]
            for slot in slots:
                total = total + bufs[pl.ds(slot, count), :]
            dst[spot, :] = total
        if k < last:
            for copy in stages[k]():
                copy.start()
        else:
            for stage in stages[:last]:
                for copy in stage():
                    copy.wait_send()

    return step


def block_kernel(n_row, n_col, x_hbm, a_hbm, g_hbm, w1, w2, x_buf, full,
                 g_buf, a_buf, g4, d4, band1, band2, w9, acc1, acc2, dz0, dz1, zp, xp,
                 s_g, s_a, s_e, s_o, gcol, acol, dcol,
                 strip, pack_l, pack_r, rl, rr, corners, data, bufs0, bufs1, bufs2,
                 in_sem, loc_sem, hsend_sem, hrecv_sem, send_sem, recv_sem):
    row, col = lax.axis_index("row"), lax.axis_index("col")
    x, core, z, y = row // 2, row % 2, col // 2, col % 2
    x_peer, y_peer = (col, 2 * (1 - x) + core), (2 * z + 1 - y, row)
    core_peer = (col, 2 * x + 1 - core)
    z_peers = [(2 * ((z + t) % 4) + y, row) for t in (1, 2, 3)]
    xy_peers = [(y_peer[0], x_peer[1]), y_peer, x_peer]
    place = (core, 2 * x + y, z, core_peer, xy_peers, z_peers)
    chain0, chain1, chain2 = (make_chain(*rows, CHAIN_SEMS * k, data, full, bufs, send_sem, recv_sem, place)
                              for k, (rows, bufs) in enumerate(zip(CHAINS, (bufs0, bufs1, bufs2))))

    has_n, has_s, has_w, has_e = row > 0, row < n_row - 1, col > 0, col < n_col - 1
    dirs = {
        "n": (has_n, row - 1, col), "s": (has_s, row + 1, col),
        "w": (has_w, row, col - 1), "e": (has_e, row, col + 1),
        "nw": (has_n & has_w, row - 1, col - 1), "ne": (has_n & has_e, row - 1, col + 1),
        "sw": (has_s & has_w, row + 1, col - 1), "se": (has_s & has_e, row + 1, col + 1),
    }
    barrier = pltpu.get_barrier_semaphore()
    for ok, r, c in dirs.values():
        @pl.when(ok)
        def _(r=r, c=c):
            pl.semaphore_signal(barrier, inc=1, device_id=(c, r), device_id_type=MESH)
    for peer in (core_peer, *xy_peers, *z_peers):
        pl.semaphore_signal(barrier, inc=1, device_id=peer, device_id_type=MESH)
    strips = [pltpu.make_async_copy(src.at[:, :, pl.ds(c0, 16), :], strip.at[k], loc_sem.at[k])
              for k, (src, c0) in enumerate(((g_hbm, 0), (g_hbm, COLS - 16), (a_hbm, 0), (a_hbm, COLS - 16)))]
    for cp in strips:
        cp.start()
    loads = [[pltpu.make_async_copy(src.at[m], dst, in_sem.at[m, j]) for j, (src, dst) in enumerate((
        (g_hbm, g_buf.at[m, pl.ds(2, ROWS)]), (a_hbm, a_buf.at[m, pl.ds(1, ROWS)]), (x_hbm, x_buf.at[m])))] for m in range(IMGS)]
    for j in range(3):
        for m in range(IMGS):
            loads[m][j].start()
    for ok, views in ((has_n, [g_buf.at[:, pl.ds(0, 2)], a_buf.at[:, pl.ds(0, 1)]]),
                      (has_s, [g_buf.at[:, pl.ds(ROWS + 2, 2)], a_buf.at[:, pl.ds(ROWS + 1, 1)]]),
                      (has_w, [rl]), (has_e, [rr]),
                      (dirs["nw"][0], [corners.at[0]]), (dirs["ne"][0], [corners.at[1]]),
                      (dirs["sw"][0], [corners.at[2]]), (dirs["se"][0], [corners.at[3]])):
        @pl.when(jnp.logical_not(ok))
        def _(views=views):
            for view in views:
                view[...] = jnp.zeros(view.shape, BF16)
    n_s, w_e = has_n.astype(jnp.int32) + has_s.astype(jnp.int32), has_w.astype(jnp.int32) + has_e.astype(jnp.int32)
    pl.semaphore_wait(barrier, n_s + w_e + n_s * w_e + 7)

    copies = [
        ("s", "n", g_hbm.at[:, pl.ds(ROWS - 2, 2)], g_buf.at[:, pl.ds(0, 2)]),
        ("n", "s", g_hbm.at[:, pl.ds(0, 2)], g_buf.at[:, pl.ds(ROWS + 2, 2)]),
        ("s", "n", a_hbm.at[:, pl.ds(ROWS - 1, 1)], a_buf.at[:, pl.ds(0, 1)]),
        ("n", "s", a_hbm.at[:, pl.ds(0, 1)], a_buf.at[:, pl.ds(ROWS + 1, 1)]),
        ("e", "w", pack_r, rl),
        ("w", "e", pack_l, rr),
        ("se", "nw", pack_r.at[:, :, pl.ds(32, 16)], corners.at[0]),
        ("sw", "ne", pack_l.at[:, :, pl.ds(32, 16)], corners.at[1]),
        ("ne", "sw", pack_r.at[:, :, pl.ds(0, 16)], corners.at[2]),
        ("nw", "se", pack_l.at[:, :, pl.ds(0, 16)], corners.at[3]),
    ]

    def rcopy(k, where):
        _, r, c = dirs[where]
        return pltpu.make_async_remote_copy(src_ref=copies[k][2], dst_ref=copies[k][3], send_sem=hsend_sem.at[k],
                                            recv_sem=hrecv_sem.at[k], device_id=(c, r), device_id_type=MESH)

    def start_halo(k):
        @pl.when(dirs[copies[k][0]][0])
        def _():
            rcopy(k, copies[k][0]).start()

    for k in range(4):
        start_halo(k)
    for k in range(4):
        strips[k].wait()
        pack = pack_l if k % 2 == 0 else pack_r
        for m in range(IMGS):
            s_g[pl.ds(0, ROWS * 16), :] = strip[k, m].astype(F32).reshape(ROWS * 16, CH)
            for slot, first_col in (((0, 0 if k == 0 else 14), (1, 1 if k == 0 else 15)) if k < 2 else ((2, 0 if k == 2 else 15),)):
                pack[m, slot] = s_g[pl.ds(first_col, ROWS, stride=16), :].astype(BF16)
    for k in range(4, 10):
        start_halo(k)

    for w, band in ((w1, band1), (w2, band2)):
        for dri in range(3):
            band[pl.ds(dri * 512 + 384, CH), LO] = jnp.zeros((CH, CH), BF16)
            band[pl.ds(dri * 512, CH), HI] = jnp.zeros((CH, CH), BF16)
        for a in range(3):
            for c in range(3):
                tap = w[a, c].astype(F32).T.astype(BF16)
                dri = 2 - a
                band[pl.ds(dri * 512 + (2 - c) * CH, CH), LO] = tap
                band[pl.ds(dri * 512 + (3 - c) * CH, CH), HI] = tap
                if w is w2:
                    w9[pl.ds((dri * 3 + 2 - c) * CH, CH), :] = tap
    acc1[...] = jnp.zeros_like(acc1)
    acc2[...] = jnp.zeros_like(acc2)

    def window_row(m, r, t):
        base = t * 208
        s_g[pl.ds(base + 8, COLS), :] = g_buf[m, r].astype(F32)
        at = pl.multiple_of((m * G_ROWS + r) * HALF, TILE)
        for q in range(4):
            g4[pl.ds(at, HALF), pl.ds(q * CH, CH)] = s_g[pl.ds(base + 7 + q, HALF, stride=2), :].astype(BF16)

    def build_g4(n, carry):
        for t in range(4):
            window_row(n // 12, 2 + (n % 12) * 4 + t, t)
        return carry

    def prep_x(n, carry):
        m, r0 = n // PER, (n % PER) * STEP
        at = pl.multiple_of(n * STEP * HALF, TILE)
        for t in range(STEP):
            s_a[pl.ds(t * COLS, COLS), :] = x_buf[m, r0 + t].astype(F32)
            for q in range(2):
                xp[pl.ds(at + t * HALF, HALF), pl.ds(q * CH, CH)] = s_a[pl.ds(t * COLS + q, HALF, stride=2), :].astype(BF16)
        return carry

    s_g[...] = jnp.zeros_like(s_g)
    for m in range(IMGS):
        loads[m][0].wait()
    lax.fori_loop(0, 24, build_g4, 0)
    for m in range(IMGS):
        loads[m][2].wait()
    lax.fori_loop(0, CHUNKS, prep_x, 0)

    for k in range(10):
        to, frm = copies[k][:2]
        @pl.when(dirs[to][0])
        def _():
            rcopy(k, to).wait_send()
        @pl.when(dirs[frm][0])
        def _():
            rcopy(k, frm).wait_recv()

    for side, (beside, top, bot) in enumerate(((rl, 0, 2), (rr, 1, 3))):
        for m in range(IMGS):
            for k in range(2):
                slot = k if side == 0 else k + 1
                gcol[side, m, slot, pl.ds(8, ROWS), :] = beside[m, k].astype(F32)
                gcol[side, m, slot, pl.ds(6, 2), :] = corners[top, m, k].astype(F32)[14:16]
                gcol[side, m, slot, pl.ds(8 + ROWS, 2), :] = corners[bot, m, k].astype(F32)[0:2]
            acol[side, m, pl.ds(8, ROWS), :] = beside[m, 2].astype(F32)
            acol[side, m, pl.ds(7, 1), :] = corners[top, m, 2].astype(F32)[15:16]
            acol[side, m, pl.ds(8 + ROWS, 1), :] = corners[bot, m, 2].astype(F32)[0:1]
    for m in range(IMGS):
        for side in range(2):
            edge = g_buf[m, :, pl.ds(0 if side == 0 else COLS - 16, 16), :].astype(F32)
            s_g[pl.ds(0, G_ROWS * 16), :] = edge.reshape(G_ROWS * 16, CH)
            gcol[side, m, 2 if side == 0 else 0, pl.ds(6, G_ROWS), :] = s_g[pl.ds(0 if side == 0 else 15, G_ROWS, stride=16), :]
    lhs = jnp.concatenate([jnp.concatenate(
        [gcol[side, m, dci, pl.ds(6 + dri, 64), :].astype(BF16) for dri in range(3) for dci in range(3)], axis=1)
        for side in range(2) for m in range(IMGS)], axis=0)
    dz_col = jnp.dot(lhs, w9[...], preferred_element_type=F32)
    for side, inside in ((0, has_w), (1, has_e)):
        for m in range(IMGS):
            _, slope = gelu_both(acol[side, m, pl.ds(7, 64), :])
            first_row = (side * IMGS + m) * 64
            dcol[side, m] = jnp.where(inside, dz_col[first_row:first_row + 64] * slope, 0.0)

    for m in range(IMGS):
        for t, r in enumerate((0, 1, G_ROWS - 2, G_ROWS - 1)):
            window_row(m, r, t)
    line = lax.broadcasted_iota(jnp.int32, (16, CH), 0)

    def patch(n, carry):
        for t in range(4):
            for m in range(IMGS):
                r = n * 4 + t
                at = pl.multiple_of((m * G_ROWS + r) * HALF, TILE)
                for side, where, q, hit in ((0, at, 0, 0), (1, at + HALF - 16, 3, 15)):
                    spot = (pl.ds(pl.multiple_of(where, 16), 16), pl.ds(q * CH, CH))
                    new = jnp.broadcast_to(gcol[side, m, 1, pl.ds(6 + r, 1), :], (16, CH))
                    g4[spot] = jnp.where(line == hit, new, g4[spot].astype(F32)).astype(BF16)
        return carry

    lax.fori_loop(0, 13, patch, 0)
    for m in range(IMGS):
        loads[m][1].wait()

    def g_rows(m, r, count):
        return g4[pl.ds(pl.multiple_of((m * G_ROWS + r) * HALF, TILE), count * HALF), :]

    def d_rows(m, r, count):
        return d4[pl.ds(pl.multiple_of((m * A_ROWS + r) * HALF, TILE), count * HALF), :]

    def one_row(m, d, t, dz, inside):
        turn = t % TURNS
        base = turn * COLS
        s_a[pl.ds(base, COLS), :] = a_buf[m, d].astype(F32)
        at = pl.multiple_of((m * A_ROWS + d) * HALF, TILE)
        z_e, slope_e = gelu_both(s_a[pl.ds(base, HALF, stride=2), :])
        z_o, slope_o = gelu_both(s_a[pl.ds(base + 1, HALF, stride=2), :])
        if inside:
            z_at = pl.multiple_of((m * ROWS + d - 1) * HALF, TILE)
            zp[pl.ds(z_at, HALF), LO] = z_e.astype(BF16)
            zp[pl.ds(z_at, HALF), HI] = z_o.astype(BF16)
        da_e = dz[pl.ds(t * HALF, HALF), LO] * slope_e
        da_o = dz[pl.ds(t * HALF, HALF), HI] * slope_o
        s_e[turn, pl.ds(8, HALF), :] = da_e
        s_o[turn, pl.ds(8, HALF), :] = da_o
        s_o[turn, pl.ds(7, 1), :] = dcol[0, m, pl.ds(d, 1), :]
        s_e[turn, pl.ds(8 + HALF, 1), :] = dcol[1, m, pl.ds(d, 1), :]
        d4[pl.ds(at, HALF), LO] = s_o[turn, pl.ds(7, HALF), :].astype(BF16)
        d4[pl.ds(at, HALF), HI] = da_e.astype(BF16)
        d4[pl.ds(at, HALF), pl.ds(2 * CH, CH)] = da_o.astype(BF16)
        d4[pl.ds(at, HALF), pl.ds(3 * CH, CH)] = s_e[turn, pl.ds(9, HALF), :].astype(BF16)

    frame = [(m, d) for m in range(IMGS) for d in (0, A_ROWS - 1)]
    lhs = jnp.concatenate([jnp.concatenate([g_rows(m, d + t, 1) for t in range(3)], axis=1) for m, d in frame], axis=0)
    matmul_halves(lhs, band2[...], dz0)
    for t, (m, d) in enumerate(frame):
        one_row(m, d, t, dz0, False)
    for edge, ok in ((0, has_n), (A_ROWS - 1, has_s)):
        @pl.when(jnp.logical_not(ok))
        def _(edge=edge):
            for m in range(IMGS):
                d4[pl.ds((m * A_ROWS + edge) * HALF, HALF), :] = jnp.zeros((HALF, 4 * CH), BF16)

    def conv_a(n, out):
        m, r0 = n // A_PER, (n % A_PER) * A_STEP
        lhs = jnp.concatenate([g_rows(m, r0 + 1 + t, A_STEP) for t in range(3)], axis=1)
        matmul_halves(lhs, band2[...], out)

    conv_a(0, dz0)

    def step_a(i, carry):
        for k in range(A_UNROLL):
            n = A_UNROLL * i + k
            m, r0 = n // A_PER, (n % A_PER) * A_STEP
            dz, dz_next = ((dz0, dz1), (dz1, dz0))[k % 2] if A_UNROLL > 1 else (dz0, dz0)
            for t in range(A_STEP):
                one_row(m, r0 + 1 + t, t, dz, True)
            conv_a(jnp.minimum(n + 1, IMGS * A_PER - 1), dz_next)
        return carry

    lax.fori_loop(0, IMGS * A_PER // A_UNROLL, step_a, 0)

    def grad(i, pairs, windows, skip, dris, acc):
        m, r0 = i // 3, (i % 3) * 2 * STEP
        win = jnp.concatenate([windows(m, r0 + skip + t, 2 * STEP) for t in dris], axis=1)
        rows = pairs[pl.ds(pl.multiple_of(i * 2 * STEP * HALF, TILE), 2 * STEP * HALF), :]
        spot = pl.ds(dris[0] * WIN, len(dris) * WIN)
        acc[:, spot] += lax.dot_general(rows, win, BY_ROWS, preferred_element_type=F32)

    def step_z(i, carry):
        for t in range(3):
            grad(3 * i + t, zp, g_rows, 1, (0, 1, 2), acc2)
        return carry

    lax.fori_loop(0, IMGS, step_z, 0)

    def fold(acc, a, at):
        for c in range(3):
            left, top = (2 - a) * WIN + (2 - c) * CH, at + c * CH
            data[pl.ds(top, CH), :] = acc[LO, pl.ds(left, CH)] + acc[HI, pl.ds(left + CH, CH)]

    for a in range(3):
        fold(acc2, a, a * TAP_ROWS)
    chain0(0)

    def at_steps(i, table):
        for when, chain, k in table:
            def run(_, carry, chain=chain, k=k):
                chain(k)
                return carry

            lax.fori_loop(0, (i == when).astype(jnp.int32), run, 0)

    def step_b(i, carry):
        at_steps(i, ((1, chain0, 1),))
        for t in range(3):
            grad(3 * i + t, xp, d_rows, 0, (0, 1), acc1)
        return carry

    def step_b2(i, carry):
        at_steps(i, ((1, chain0, 2), (1, chain1, 1)))
        for t in range(3):
            grad(3 * i + t, xp, d_rows, 0, (2,), acc1)
        return carry

    lax.fori_loop(0, IMGS, step_b, 0)
    fold(acc1, 1, 3 * TAP_ROWS)
    fold(acc1, 2, 4 * TAP_ROWS)
    chain1(0)
    lax.fori_loop(0, IMGS, step_b2, 0)
    fold(acc1, 0, 5 * TAP_ROWS)
    chain2(0)

    def conv_x(n, out):
        m, r0 = n // PER, (n % PER) * STEP
        win = jnp.concatenate([d_rows(m, r0 + t, STEP) for t in range(3)], axis=1)
        matmul_halves(win, band1[...], out)

    def finish(n, dz):
        m, r0 = n // PER, (n % PER) * STEP
        own = g4[pl.ds(pl.multiple_of((m * G_ROWS + r0 + 2) * HALF, TILE), STEP * HALF), pl.ds(CH, 2 * CH)].astype(F32)
        for t in range(STEP):
            part = dz[pl.ds(t * HALF, HALF), :] + own[t * HALF:(t + 1) * HALF]
            for q in range(2):
                s_a[pl.ds(t * COLS + q, HALF, stride=2), :] = part[:, q * CH:(q + 1) * CH]
            x_buf[m, r0 + t] = s_a[pl.ds(t * COLS, COLS), :].astype(BF16)

    conv_x(0, dz0)

    def step_c(i, carry):
        at_steps(i, ((1, chain0, 3), (3, chain0, 4), (4, chain1, 4), (5, chain0, 5)))
        conv_x(2 * i + 1, dz1)
        finish(2 * i, dz0)
        at_steps(i, ((0, chain2, 1), (0, chain1, 2), (2, chain2, 2), (2, chain1, 3), (4, chain2, 3)))
        conv_x(jnp.minimum(2 * i + 2, CHUNKS - 1), dz0)
        finish(2 * i + 1, dz1)
        return carry

    lax.fori_loop(0, CHUNKS // 2, step_c, 0)
    for chain, k in ((chain1, 5), (chain2, 4), (chain0, 6), (chain1, 6), (chain2, 5), (chain2, 6)):
        chain(k)


def place_kernel(dx_in, dw_in, dx_out, dw1_out, dw2_out, out_sem):
    pieces = [(dx_in.at[m], dx_out.at[m]) for m in range(IMGS)]
    for dst, at, first, count in ((dw2_out, 0, 0, 3), (dw1_out, 5, 0, 1), (dw1_out, 3, 1, 2)):
        pieces.append((dw_in.at[pl.ds(at * TAP_ROWS, count * TAP_ROWS)], dst.at[pl.ds(first * TAP_ROWS, count * TAP_ROWS)]))
    stores = [pltpu.make_async_copy(src, dst, out_sem.at[k]) for k, (src, dst) in enumerate(pieces)]
    for store in stores:
        store.start()
    for store in stores:
        store.wait()


def place_results(d_x, dw):
    taps = jax.ShapeDtypeStruct((9 * CH, CH), F32)
    return pl.pallas_call(
        place_kernel,
        out_shape=[jax.ShapeDtypeStruct((IMGS, ROWS, COLS, CH), BF16), taps, taps],
        in_specs=[pl.BlockSpec(memory_space=pltpu.VMEM)] * 2,
        out_specs=[pl.BlockSpec(memory_space=pl.ANY)] * 3,
        scratch_shapes=[pltpu.SemaphoreType.DMA((5,))],
        compiler_params=pltpu.CompilerParams(vmem_limit_bytes=PLACE_BYTES),
        name="place_results",
    )(d_x, dw)


def block_grads(mesh_shape, x_tile, a_tile, g_tile, w_one, w_two):
    vm = pl.BlockSpec(memory_space=pltpu.VMEM)
    hbm = pl.BlockSpec(memory_space=pl.ANY)
    half, pair = STEP * HALF, 2 * CH
    padded, cols = (STEP, HALF + 16, CH), (IMGS, 3, ROWS, CH)
    return pl.pallas_call(
        functools.partial(block_kernel, mesh_shape["row"], mesh_shape["col"]),
        out_shape=[pltpu.VMEM((IMGS, ROWS, COLS, CH), BF16), pltpu.VMEM((18 * CH, CH), F32)],
        in_specs=[hbm] * 3 + [vm] * 2,
        out_specs=[vm] * 2,
        scratch_shapes=[pltpu.VMEM(shape, BF16) for shape in (
            (IMGS, G_ROWS, COLS, CH), (IMGS, A_ROWS, COLS, CH),
            (IMGS * G_ROWS * HALF, WIN), (IMGS * A_ROWS * HALF, WIN), (3 * WIN, pair), (3 * WIN, pair), (9 * CH, CH))
        ] + [pltpu.VMEM(shape, F32) for shape in ((pair, 3 * WIN), (pair, 3 * WIN), (half, pair), (half, pair))
        ] + [pltpu.VMEM(shape, BF16) for shape in ((CHUNKS * half, pair), (CHUNKS * half, pair))
        ] + [pltpu.VMEM(shape, F32) for shape in (
            (4 * 208 + 16, CH), (STEP * COLS, CH), padded, padded, (2, IMGS, 3, 72, CH), (2, IMGS, 72, CH), (2, IMGS, 64, CH))
        ] + [pltpu.VMEM(shape, BF16) for shape in ((4, IMGS, ROWS, 16, CH), cols, cols, cols, cols, (4, IMGS, 3, 16, CH))
        ] + [pltpu.VMEM(shape, F32) for shape in ((18 * CH, CH), *((size, CH) for _, size in CHAINS))
        ] + [pltpu.SemaphoreType.DMA(shape) for shape in ((IMGS, 3), (4,), (10,), (10,), (3 * CHAIN_SEMS,), (3 * CHAIN_SEMS,))],
        compiler_params=pltpu.CompilerParams(collective_id=0, has_side_effects=True, vmem_limit_bytes=BLOCK_BYTES),
        name="block_grads",
    )(x_tile, a_tile, g_tile, w_one, w_two)


def solution(mesh):
    shape = dict(mesh.shape)

    def local_step(x_tile, a_tile, g_tile, w_one, w_two):
        d_x, dw = block_grads(shape, x_tile, a_tile, g_tile, w_one, w_two)
        d_x, d_w1, d_w2 = place_results(d_x, dw)
        return d_x, d_w1.reshape(w_one.shape), d_w2.reshape(w_two.shape)

    tile_spec = P(None, "row", "col", None)
    return jax.shard_map(local_step, mesh=mesh, in_specs=(tile_spec, tile_spec, tile_spec, P(), P()), out_specs=(tile_spec, P(), P()), check_vma=False)
```

```python
import functools

import jax
import jax.numpy as jnp
from jax import lax
from jax.experimental import pallas as pl
from jax.experimental.pallas import tpu as pltpu
from jax.sharding import PartitionSpec as P

MESH = pl.DeviceIdType.MESH
F32 = jnp.float32
BF16 = jnp.bfloat16
IMGS = 2
ROWS = 48
COLS = 192
CH = 128
HALF = COLS // 2
G_ROWS = ROWS + 4
A_ROWS = ROWS + 2
TANH_SCALE = 0.7978845608028654
CUBE_COEF = 0.044715
STEP = 8
TILE = 32
BY_ROWS = (((0,), (0,)), ((), ()))
CHUNKS = IMGS * ROWS // STEP
PER = ROWS // STEP
CHAINS = ((0, 1024), (1024, 768), (1792, 512))
A_STEP = 6
A_PER = ROWS // A_STEP
A_UNROLL = 2
TURNS = 1
CHAIN_SEMS = 14
BLOCK_BYTES = 61145088
PLACE_BYTES = 1048576
TAP_ROWS = 3 * CH
LO, HI = pl.ds(0, CH), pl.ds(CH, CH)
WIN = 4 * CH


def gelu_both(a_val):
    sq = a_val * a_val
    tanh_val = jnp.tanh(a_val * (TANH_SCALE + (TANH_SCALE * CUBE_COEF) * sq))
    half_plus = 0.5 + 0.5 * tanh_val
    inner = (0.5 * TANH_SCALE) + (1.5 * TANH_SCALE * CUBE_COEF) * sq
    return a_val * half_plus, half_plus + ((1.0 - tanh_val * tanh_val) * a_val) * inner


def matmul_halves(lhs, rhs, out):
    count = lhs.shape[0] // 2
    for k in range(2):
        out[pl.ds(k * count, count), :] = jnp.dot(lhs[k * count:(k + 1) * count], rhs, preferred_element_type=F32)


def make_chain(base, size, first_sem, data, full, bufs, send_sem, recv_sem, place, last=6):
    core, quadrant, z, core_peer, xy_peers, z_peers = place
    half, eighth, quarter = size // 2, size // 8, size // 32
    mine0 = base + core * half
    away0 = base + half - core * half
    mine1 = mine0 + quadrant * eighth
    away1 = [mine0 + (3 - quadrant) * eighth, mine0 + (quadrant + 1 - 2 * (quadrant % 2)) * eighth,
             mine0 + (quadrant + 2 - 4 * (quadrant // 2)) * eighth]
    mine2 = mine1 + z * quarter
    away2 = [mine1 + ((z + 1 + t) % 4) * quarter for t in range(3)]
    slots1 = [half + t * eighth for t in range(3)]
    slots2 = [half + 3 * eighth + t * quarter for t in range(3)]

    def rows(ref, start, count):
        return ref.at[pl.ds(pl.multiple_of(start, 8), count)]

    def remote(src, dst, sem, peer):
        return pltpu.make_async_remote_copy(src_ref=src, dst_ref=dst, send_sem=send_sem.at[first_sem + sem],
                                            recv_sem=recv_sem.at[first_sem + sem], device_id=peer, device_id_type=MESH)

    def same(start, count, sem, peer):
        return remote(rows(full, start, count), rows(full, start, count), sem, peer)

    stages = [
        lambda: [remote(rows(data, away0, half), rows(bufs, 0, half), 0, core_peer)],
        lambda: [remote(rows(data, away1[t], eighth), rows(bufs, slots1[t], eighth), 1 + t, xy_peers[t]) for t in range(3)],
        lambda: [remote(rows(data, away2[t], quarter), rows(bufs, slots2[t], quarter), 4 + t, z_peers[t]) for t in range(3)],
        lambda: [same(mine2, quarter, 7 + t, z_peers[t]) for t in range(3)],
        lambda: [same(mine1, eighth, 10 + t, xy_peers[t]) for t in range(3)],
        lambda: [same(mine0, half, 13, core_peer)],
    ]
    adds = [(data, mine0, half, [0]), (data, mine1, eighth, slots1), (full, mine2, quarter, slots2)]

    def step(k):
        if k > 0:
            for copy in stages[k - 1]():
                copy.wait_recv()
        if 0 < k <= len(adds):
            dst, start, count, slots = adds[k - 1]
            spot = pl.ds(pl.multiple_of(start, 8), count)
            total = data[spot, :]
            for slot in slots:
                total = total + bufs[pl.ds(slot, count), :]
            dst[spot, :] = total
        if k < last:
            for copy in stages[k]():
                copy.start()
        else:
            for stage in stages[:last]:
                for copy in stage():
                    copy.wait_send()

    return step


def block_kernel(n_row, n_col, x_hbm, a_hbm, g_hbm, w1, w2, x_buf, full,
                 g_buf, a_buf, g4, d4, band1, band2, w9, acc1, acc2, dz0, dz1, zp, xp,
                 s_g, s_a, s_e, s_o, gcol, acol, dcol,
                 strip, pack_l, pack_r, rl, rr, corners, data, bufs0, bufs1, bufs2,
                 in_sem, loc_sem, hsend_sem, hrecv_sem, send_sem, recv_sem):
    row, col = lax.axis_index("row"), lax.axis_index("col")
    x, core, z, y = row // 2, row % 2, col // 2, col % 2
    x_peer, y_peer = (col, 2 * (1 - x) + core), (2 * z + 1 - y, row)
    core_peer = (col, 2 * x + 1 - core)
    z_peers = [(2 * ((z + t) % 4) + y, row) for t in (1, 2, 3)]
    xy_peers = [(y_peer[0], x_peer[1]), y_peer, x_peer]
    place = (core, 2 * x + y, z, core_peer, xy_peers, z_peers)
    chain0, chain1, chain2 = (make_chain(*rows, CHAIN_SEMS * k, data, full, bufs, send_sem, recv_sem, place)
                              for k, (rows, bufs) in enumerate(zip(CHAINS, (bufs0, bufs1, bufs2))))

    has_n, has_s, has_w, has_e = row > 0, row < n_row - 1, col > 0, col < n_col - 1
    dirs = {
        "n": (has_n, row - 1, col), "s": (has_s, row + 1, col),
        "w": (has_w, row, col - 1), "e": (has_e, row, col + 1),
        "nw": (has_n & has_w, row - 1, col - 1), "ne": (has_n & has_e, row - 1, col + 1),
        "sw": (has_s & has_w, row + 1, col - 1), "se": (has_s & has_e, row + 1, col + 1),
    }
    barrier = pltpu.get_barrier_semaphore()
    for ok, r, c in dirs.values():
        @pl.when(ok)
        def _(r=r, c=c):
            pl.semaphore_signal(barrier, inc=1, device_id=(c, r), device_id_type=MESH)
    for peer in (core_peer, *xy_peers, *z_peers):
        pl.semaphore_signal(barrier, inc=1, device_id=peer, device_id_type=MESH)
    strips = [pltpu.make_async_copy(src.at[:, :, pl.ds(c0, 16), :], strip.at[k], loc_sem.at[k])
              for k, (src, c0) in enumerate(((g_hbm, 0), (g_hbm, COLS - 16), (a_hbm, 0), (a_hbm, COLS - 16)))]
    for cp in strips:
        cp.start()
    loads = [[pltpu.make_async_copy(src.at[m], dst, in_sem.at[m, j]) for j, (src, dst) in enumerate((
        (g_hbm, g_buf.at[m, pl.ds(2, ROWS)]), (a_hbm, a_buf.at[m, pl.ds(1, ROWS)]), (x_hbm, x_buf.at[m])))] for m in range(IMGS)]
    for j in range(3):
        for m in range(IMGS):
            loads[m][j].start()
    for ok, views in ((has_n, [g_buf.at[:, pl.ds(0, 2)], a_buf.at[:, pl.ds(0, 1)]]),
                      (has_s, [g_buf.at[:, pl.ds(ROWS + 2, 2)], a_buf.at[:, pl.ds(ROWS + 1, 1)]]),
                      (has_w, [rl]), (has_e, [rr]),
                      (dirs["nw"][0], [corners.at[0]]), (dirs["ne"][0], [corners.at[1]]),
                      (dirs["sw"][0], [corners.at[2]]), (dirs["se"][0], [corners.at[3]])):
        @pl.when(jnp.logical_not(ok))
        def _(views=views):
            for view in views:
                view[...] = jnp.zeros(view.shape, BF16)
    n_s, w_e = has_n.astype(jnp.int32) + has_s.astype(jnp.int32), has_w.astype(jnp.int32) + has_e.astype(jnp.int32)
    pl.semaphore_wait(barrier, n_s + w_e + n_s * w_e + 7)

    copies = [
        ("s", "n", g_hbm.at[:, pl.ds(ROWS - 2, 2)], g_buf.at[:, pl.ds(0, 2)]),
        ("n", "s", g_hbm.at[:, pl.ds(0, 2)], g_buf.at[:, pl.ds(ROWS + 2, 2)]),
        ("s", "n", a_hbm.at[:, pl.ds(ROWS - 1, 1)], a_buf.at[:, pl.ds(0, 1)]),
        ("n", "s", a_hbm.at[:, pl.ds(0, 1)], a_buf.at[:, pl.ds(ROWS + 1, 1)]),
        ("e", "w", pack_r, rl),
        ("w", "e", pack_l, rr),
        ("se", "nw", pack_r.at[:, :, pl.ds(32, 16)], corners.at[0]),
        ("sw", "ne", pack_l.at[:, :, pl.ds(32, 16)], corners.at[1]),
        ("ne", "sw", pack_r.at[:, :, pl.ds(0, 16)], corners.at[2]),
        ("nw", "se", pack_l.at[:, :, pl.ds(0, 16)], corners.at[3]),
    ]

    def rcopy(k, where):
        _, r, c = dirs[where]
        return pltpu.make_async_remote_copy(src_ref=copies[k][2], dst_ref=copies[k][3], send_sem=hsend_sem.at[k],
                                            recv_sem=hrecv_sem.at[k], device_id=(c, r), device_id_type=MESH)

    def start_halo(k):
        @pl.when(dirs[copies[k][0]][0])
        def _():
            rcopy(k, copies[k][0]).start()

    for k in range(4):
        start_halo(k)
    for k in range(4):
        strips[k].wait()
        pack = pack_l if k % 2 == 0 else pack_r
        for m in range(IMGS):
            s_g[pl.ds(0, ROWS * 16), :] = strip[k, m].astype(F32).reshape(ROWS * 16, CH)
            for slot, first_col in (((0, 0 if k == 0 else 14), (1, 1 if k == 0 else 15)) if k < 2 else ((2, 0 if k == 2 else 15),)):
                pack[m, slot] = s_g[pl.ds(first_col, ROWS, stride=16), :].astype(BF16)
    for k in range(4, 10):
        start_halo(k)

    for w, band in ((w1, band1), (w2, band2)):
        for dri in range(3):
            band[pl.ds(dri * 512 + 384, CH), LO] = jnp.zeros((CH, CH), BF16)
            band[pl.ds(dri * 512, CH), HI] = jnp.zeros((CH, CH), BF16)
        for a in range(3):
            for c in range(3):
                tap = w[a, c].astype(F32).T.astype(BF16)
                dri = 2 - a
                band[pl.ds(dri * 512 + (2 - c) * CH, CH), LO] = tap
                band[pl.ds(dri * 512 + (3 - c) * CH, CH), HI] = tap
                if w is w2:
                    w9[pl.ds((dri * 3 + 2 - c) * CH, CH), :] = tap
    acc1[...] = jnp.zeros_like(acc1)
    acc2[...] = jnp.zeros_like(acc2)

    def window_row(m, r, t):
        base = t * 208
        s_g[pl.ds(base + 8, COLS), :] = g_buf[m, r].astype(F32)
        at = pl.multiple_of((m * G_ROWS + r) * HALF, TILE)
        for q in range(4):
            g4[pl.ds(at, HALF), pl.ds(q * CH, CH)] = s_g[pl.ds(base + 7 + q, HALF, stride=2), :].astype(BF16)

    def build_g4(n, carry):
        for t in range(4):
            window_row(n // 12, 2 + (n % 12) * 4 + t, t)
        return carry

    def prep_x(n, carry):
        m, r0 = n // PER, (n % PER) * STEP
        at = pl.multiple_of(n * STEP * HALF, TILE)
        for t in range(STEP):
            s_a[pl.ds(t * COLS, COLS), :] = x_buf[m, r0 + t].astype(F32)
            for q in range(2):
                xp[pl.ds(at + t * HALF, HALF), pl.ds(q * CH, CH)] = s_a[pl.ds(t * COLS + q, HALF, stride=2), :].astype(BF16)
        return carry

    s_g[...] = jnp.zeros_like(s_g)
    for m in range(IMGS):
        loads[m][0].wait()
    lax.fori_loop(0, 24, build_g4, 0)
    for m in range(IMGS):
        loads[m][2].wait()
    lax.fori_loop(0, CHUNKS, prep_x, 0)

    for k in range(10):
        to, frm = copies[k][:2]
        @pl.when(dirs[to][0])
        def _():
            rcopy(k, to).wait_send()
        @pl.when(dirs[frm][0])
        def _():
            rcopy(k, frm).wait_recv()

    for side, (beside, top, bot) in enumerate(((rl, 0, 2), (rr, 1, 3))):
        for m in range(IMGS):
            for k in range(2):
                slot = k if side == 0 else k + 1
                gcol[side, m, slot, pl.ds(8, ROWS), :] = beside[m, k].astype(F32)
                gcol[side, m, slot, pl.ds(6, 2), :] = corners[top, m, k].astype(F32)[14:16]
                gcol[side, m, slot, pl.ds(8 + ROWS, 2), :] = corners[bot, m, k].astype(F32)[0:2]
            acol[side, m, pl.ds(8, ROWS), :] = beside[m, 2].astype(F32)
            acol[side, m, pl.ds(7, 1), :] = corners[top, m, 2].astype(F32)[15:16]
            acol[side, m, pl.ds(8 + ROWS, 1), :] = corners[bot, m, 2].astype(F32)[0:1]
    for m in range(IMGS):
        for side in range(2):
            edge = g_buf[m, :, pl.ds(0 if side == 0 else COLS - 16, 16), :].astype(F32)
            s_g[pl.ds(0, G_ROWS * 16), :] = edge.reshape(G_ROWS * 16, CH)
            gcol[side, m, 2 if side == 0 else 0, pl.ds(6, G_ROWS), :] = s_g[pl.ds(0 if side == 0 else 15, G_ROWS, stride=16), :]
    lhs = jnp.concatenate([jnp.concatenate(
        [gcol[side, m, dci, pl.ds(6 + dri, 64), :].astype(BF16) for dri in range(3) for dci in range(3)], axis=1)
        for side in range(2) for m in range(IMGS)], axis=0)
    dz_col = jnp.dot(lhs, w9[...], preferred_element_type=F32)
    for side, inside in ((0, has_w), (1, has_e)):
        for m in range(IMGS):
            _, slope = gelu_both(acol[side, m, pl.ds(7, 64), :])
            first_row = (side * IMGS + m) * 64
            dcol[side, m] = jnp.where(inside, dz_col[first_row:first_row + 64] * slope, 0.0)

    for m in range(IMGS):
        for t, r in enumerate((0, 1, G_ROWS - 2, G_ROWS - 1)):
            window_row(m, r, t)
    line = lax.broadcasted_iota(jnp.int32, (16, CH), 0)

    def patch(n, carry):
        for t in range(4):
            for m in range(IMGS):
                r = n * 4 + t
                at = pl.multiple_of((m * G_ROWS + r) * HALF, TILE)
                for side, where, q, hit in ((0, at, 0, 0), (1, at + HALF - 16, 3, 15)):
                    spot = (pl.ds(pl.multiple_of(where, 16), 16), pl.ds(q * CH, CH))
                    new = jnp.broadcast_to(gcol[side, m, 1, pl.ds(6 + r, 1), :], (16, CH))
                    g4[spot] = jnp.where(line == hit, new, g4[spot].astype(F32)).astype(BF16)
        return carry

    lax.fori_loop(0, 13, patch, 0)
    for m in range(IMGS):
        loads[m][1].wait()

    def g_rows(m, r, count):
        return g4[pl.ds(pl.multiple_of((m * G_ROWS + r) * HALF, TILE), count * HALF), :]

    def d_rows(m, r, count):
        return d4[pl.ds(pl.multiple_of((m * A_ROWS + r) * HALF, TILE), count * HALF), :]

    def one_row(m, d, t, dz, inside):
        turn = t % TURNS
        base = turn * COLS
        s_a[pl.ds(base, COLS), :] = a_buf[m, d].astype(F32)
        at = pl.multiple_of((m * A_ROWS + d) * HALF, TILE)
        z_e, slope_e = gelu_both(s_a[pl.ds(base, HALF, stride=2), :])
        z_o, slope_o = gelu_both(s_a[pl.ds(base + 1, HALF, stride=2), :])
        if inside:
            z_at = pl.multiple_of((m * ROWS + d - 1) * HALF, TILE)
            zp[pl.ds(z_at, HALF), LO] = z_e.astype(BF16)
            zp[pl.ds(z_at, HALF), HI] = z_o.astype(BF16)
        da_e = dz[pl.ds(t * HALF, HALF), LO] * slope_e
        da_o = dz[pl.ds(t * HALF, HALF), HI] * slope_o
        s_e[turn, pl.ds(8, HALF), :] = da_e
        s_o[turn, pl.ds(8, HALF), :] = da_o
        s_o[turn, pl.ds(7, 1), :] = dcol[0, m, pl.ds(d, 1), :]
        s_e[turn, pl.ds(8 + HALF, 1), :] = dcol[1, m, pl.ds(d, 1), :]
        d4[pl.ds(at, HALF), LO] = s_o[turn, pl.ds(7, HALF), :].astype(BF16)
        d4[pl.ds(at, HALF), HI] = da_e.astype(BF16)
        d4[pl.ds(at, HALF), pl.ds(2 * CH, CH)] = da_o.astype(BF16)
        d4[pl.ds(at, HALF), pl.ds(3 * CH, CH)] = s_e[turn, pl.ds(9, HALF), :].astype(BF16)

    frame = [(m, d) for m in range(IMGS) for d in (0, A_ROWS - 1)]
    lhs = jnp.concatenate([jnp.concatenate([g_rows(m, d + t, 1) for t in range(3)], axis=1) for m, d in frame], axis=0)
    matmul_halves(lhs, band2[...], dz0)
    for t, (m, d) in enumerate(frame):
        one_row(m, d, t, dz0, False)
    for edge, ok in ((0, has_n), (A_ROWS - 1, has_s)):
        @pl.when(jnp.logical_not(ok))
        def _(edge=edge):
            for m in range(IMGS):
                d4[pl.ds((m * A_ROWS + edge) * HALF, HALF), :] = jnp.zeros((HALF, 4 * CH), BF16)

    def conv_a(n, out):
        m, r0 = n // A_PER, (n % A_PER) * A_STEP
        lhs = jnp.concatenate([g_rows(m, r0 + 1 + t, A_STEP) for t in range(3)], axis=1)
        matmul_halves(lhs, band2[...], out)

    conv_a(0, dz0)

    def step_a(i, carry):
        for k in range(A_UNROLL):
            n = A_UNROLL * i + k
            m, r0 = n // A_PER, (n % A_PER) * A_STEP
            dz, dz_next = ((dz0, dz1), (dz1, dz0))[k % 2] if A_UNROLL > 1 else (dz0, dz0)
            for t in range(A_STEP):
                one_row(m, r0 + 1 + t, t, dz, True)
            conv_a(jnp.minimum(n + 1, IMGS * A_PER - 1), dz_next)
        return carry

    lax.fori_loop(0, IMGS * A_PER // A_UNROLL, step_a, 0)

    def grad(i, pairs, windows, skip, dris, acc):
        m, r0 = i // 3, (i % 3) * 2 * STEP
        win = jnp.concatenate([windows(m, r0 + skip + t, 2 * STEP) for t in dris], axis=1)
        rows = pairs[pl.ds(pl.multiple_of(i * 2 * STEP * HALF, TILE), 2 * STEP * HALF), :]
        spot = pl.ds(dris[0] * WIN, len(dris) * WIN)
        acc[:, spot] += lax.dot_general(rows, win, BY_ROWS, preferred_element_type=F32)

    def step_z(i, carry):
        for t in range(3):
            grad(3 * i + t, zp, g_rows, 1, (0, 1, 2), acc2)
        return carry

    lax.fori_loop(0, IMGS, step_z, 0)

    def fold(acc, a, at):
        for c in range(3):
            left, top = (2 - a) * WIN + (2 - c) * CH, at + c * CH
            data[pl.ds(top, CH), :] = acc[LO, pl.ds(left, CH)] + acc[HI, pl.ds(left + CH, CH)]

    for a in range(3):
        fold(acc2, a, a * TAP_ROWS)
    chain0(0)

    def at_steps(i, table):
        for when, chain, k in table:
            def run(_, carry, chain=chain, k=k):
                chain(k)
                return carry

            lax.fori_loop(0, (i == when).astype(jnp.int32), run, 0)

    def step_b(i, carry):
        at_steps(i, ((1, chain0, 1),))
        for t in range(3):
            grad(3 * i + t, xp, d_rows, 0, (0, 1), acc1)
        return carry

    def step_b2(i, carry):
        at_steps(i, ((1, chain0, 2), (1, chain1, 1)))
        for t in range(3):
            grad(3 * i + t, xp, d_rows, 0, (2,), acc1)
        return carry

    lax.fori_loop(0, IMGS, step_b, 0)
    fold(acc1, 1, 3 * TAP_ROWS)
    fold(acc1, 2, 4 * TAP_ROWS)
    chain1(0)
    lax.fori_loop(0, IMGS, step_b2, 0)
    fold(acc1, 0, 5 * TAP_ROWS)
    chain2(0)

    def conv_x(n, out):
        m, r0 = n // PER, (n % PER) * STEP
        win = jnp.concatenate([d_rows(m, r0 + t, STEP) for t in range(3)], axis=1)
        matmul_halves(win, band1[...], out)

    def finish(n, dz):
        m, r0 = n // PER, (n % PER) * STEP
        own = g4[pl.ds(pl.multiple_of((m * G_ROWS + r0 + 2) * HALF, TILE), STEP * HALF), pl.ds(CH, 2 * CH)].astype(F32)
        for t in range(STEP):
            part = dz[pl.ds(t * HALF, HALF), :] + own[t * HALF:(t + 1) * HALF]
            for q in range(2):
                s_a[pl.ds(t * COLS + q, HALF, stride=2), :] = part[:, q * CH:(q + 1) * CH]
            x_buf[m, r0 + t] = s_a[pl.ds(t * COLS, COLS), :].astype(BF16)

    conv_x(0, dz0)

    def step_c(i, carry):
        at_steps(i, ((1, chain0, 3), (2, chain2, 2), (3, chain0, 4), (4, chain2, 3), (5, chain0, 5)))
        conv_x(2 * i + 1, dz1)
        finish(2 * i, dz0)
        at_steps(i, ((0, chain2, 1), (0, chain1, 2), (2, chain1, 3), (4, chain1, 4), (5, chain2, 4)))
        conv_x(jnp.minimum(2 * i + 2, CHUNKS - 1), dz0)
        finish(2 * i + 1, dz1)
        return carry

    lax.fori_loop(0, CHUNKS // 2, step_c, 0)
    for chain, k in ((chain1, 5), (chain0, 6), (chain2, 5), (chain1, 6), (chain2, 6)):
        chain(k)


def place_kernel(dx_in, dw_in, dx_out, dw1_out, dw2_out, out_sem):
    pieces = [(dx_in.at[m], dx_out.at[m]) for m in range(IMGS)]
    for dst, at, first, count in ((dw2_out, 0, 0, 3), (dw1_out, 5, 0, 1), (dw1_out, 3, 1, 2)):
        pieces.append((dw_in.at[pl.ds(at * TAP_ROWS, count * TAP_ROWS)], dst.at[pl.ds(first * TAP_ROWS, count * TAP_ROWS)]))
    stores = [pltpu.make_async_copy(src, dst, out_sem.at[k]) for k, (src, dst) in enumerate(pieces)]
    for store in stores:
        store.start()
    for store in stores:
        store.wait()


def place_results(d_x, dw):
    taps = jax.ShapeDtypeStruct((9 * CH, CH), F32)
    return pl.pallas_call(
        place_kernel,
        out_shape=[jax.ShapeDtypeStruct((IMGS, ROWS, COLS, CH), BF16), taps, taps],
        in_specs=[pl.BlockSpec(memory_space=pltpu.VMEM)] * 2,
        out_specs=[pl.BlockSpec(memory_space=pl.ANY)] * 3,
        scratch_shapes=[pltpu.SemaphoreType.DMA((5,))],
        compiler_params=pltpu.CompilerParams(vmem_limit_bytes=PLACE_BYTES),
        name="place_results",
    )(d_x, dw)


def block_grads(mesh_shape, x_tile, a_tile, g_tile, w_one, w_two):
    vm = pl.BlockSpec(memory_space=pltpu.VMEM)
    hbm = pl.BlockSpec(memory_space=pl.ANY)
    half, pair = STEP * HALF, 2 * CH
    padded, cols = (STEP, HALF + 16, CH), (IMGS, 3, ROWS, CH)
    return pl.pallas_call(
        functools.partial(block_kernel, mesh_shape["row"], mesh_shape["col"]),
        out_shape=[pltpu.VMEM((IMGS, ROWS, COLS, CH), BF16), pltpu.VMEM((18 * CH, CH), F32)],
        in_specs=[hbm] * 3 + [vm] * 2,
        out_specs=[vm] * 2,
        scratch_shapes=[pltpu.VMEM(shape, BF16) for shape in (
            (IMGS, G_ROWS, COLS, CH), (IMGS, A_ROWS, COLS, CH),
            (IMGS * G_ROWS * HALF, WIN), (IMGS * A_ROWS * HALF, WIN), (3 * WIN, pair), (3 * WIN, pair), (9 * CH, CH))
        ] + [pltpu.VMEM(shape, F32) for shape in ((pair, 3 * WIN), (pair, 3 * WIN), (half, pair), (half, pair))
        ] + [pltpu.VMEM(shape, BF16) for shape in ((CHUNKS * half, pair), (CHUNKS * half, pair))
        ] + [pltpu.VMEM(shape, F32) for shape in (
            (4 * 208 + 16, CH), (STEP * COLS, CH), padded, padded, (2, IMGS, 3, 72, CH), (2, IMGS, 72, CH), (2, IMGS, 64, CH))
        ] + [pltpu.VMEM(shape, BF16) for shape in ((4, IMGS, ROWS, 16, CH), cols, cols, cols, cols, (4, IMGS, 3, 16, CH))
        ] + [pltpu.VMEM(shape, F32) for shape in ((18 * CH, CH), *((size, CH) for _, size in CHAINS))
        ] + [pltpu.SemaphoreType.DMA(shape) for shape in ((IMGS, 3), (4,), (10,), (10,), (3 * CHAIN_SEMS,), (3 * CHAIN_SEMS,))],
        compiler_params=pltpu.CompilerParams(collective_id=0, has_side_effects=True, vmem_limit_bytes=BLOCK_BYTES),
        name="block_grads",
    )(x_tile, a_tile, g_tile, w_one, w_two)


def solution(mesh):
    shape = dict(mesh.shape)

    def local_step(x_tile, a_tile, g_tile, w_one, w_two):
        d_x, dw = block_grads(shape, x_tile, a_tile, g_tile, w_one, w_two)
        d_x, d_w1, d_w2 = place_results(d_x, dw)
        return d_x, d_w1.reshape(w_one.shape), d_w2.reshape(w_two.shape)

    tile_spec = P(None, "row", "col", None)
    return jax.shard_map(local_step, mesh=mesh, in_specs=(tile_spec, tile_spec, tile_spec, P(), P()), out_specs=(tile_spec, P(), P()), check_vma=False)
```
